256 devices in a mesh: batch: 2 (over x_hi), items: 128 (over z, x_lo, y, core).
Axes of the slice: x: 4 (x_hi: 2, x_lo: 2; x = x_hi * 2 + x_lo), y: 4, z: 8, core: 2. Of those that a mesh axis runs over, the one named last changes fastest.
Arguments:
- users: bfloat16 [10240, 256], P(('batch', 'items')), may hold values from -6 to 6
- items: bfloat16 [65536, 256], P(('batch', 'items')), may hold values from -6 to 6
- pos_ids: int32 [10240], P(('batch', 'items')), may hold values from 0 to 65535
Outputs:
- loss: float32 [10240], P(('batch', 'items'))
- user_grad: float32 [10240, 256], P(('batch', 'items'))
- item_grad: float32 [65536, 256], P(('batch', 'items'))
The draws below stay inside these ranges and needn't reach their ends.
All inputs are finite; a program needn't handle non-finite values.
Results may differ from the reference program's by a relative error of at most 0.0015.
Values may be sent and summed in bfloat16 or wider, within the bound.
A program may use at most 64 MiB of HBM per device.

```python
import math
import jax
import jax.numpy as jnp
from jax import lax

E = 256
USERS = 10240
ITEMS = 65536


def joint_towers(key):
    base = jax.random.fold_in(key, 7)
    key_user, key_item, key_pick, key_flag, key_sign, key_align, key_perm = jax.random.split(base, 7)
    users = jnp.clip(jax.random.normal(key_user, (USERS, E), jnp.float32), -6.0, 6.0)
    bank = jnp.clip(0.125 * jax.random.normal(key_item, (ITEMS, E), jnp.float32), -0.75, 0.75)
    user_level = 5.0
    item_level = 320.0 / (user_level * E)
    signs = (2 * jax.random.randint(key_sign, (USERS, E), 0, 2) - 1).astype(jnp.float32)
    aligned = jax.random.randint(key_align, (USERS,), 0, 16) == 0
    users = jnp.where(aligned[:, None], user_level * signs, users)
    users = users.astype(jnp.bfloat16).astype(jnp.float32)
    order = jax.random.permutation(key_perm, ITEMS).astype(jnp.int32)
    rank = jnp.argsort(order).astype(jnp.int32)
    owned = rank < USERS
    partner = jnp.minimum(rank, USERS - 1)
    match = owned & aligned[partner]
    bank = jnp.where(match[:, None], item_level * signs[partner], bank)
    return (users, bank)


def draw_users(key, part):
    return joint_towers(key)[0].astype(jnp.bfloat16)


def draw_items(key, part):
    return joint_towers(key)[1].astype(jnp.bfloat16)


def place_ends(drawn, stream_key, least, high):
    dims = drawn.shape
    index_at = [jax.random.randint(jax.random.fold_in(stream_key, axis), (), 0, dims[axis]) for axis in range(len(dims))]
    drawn = drawn.at[tuple(index_at)].set(least)
    longest = dims.index(max(dims))
    index_at[longest] = (index_at[longest] + 1) % dims[longest]
    return drawn.at[tuple(index_at)].set(high)


def setup_inputs(seed: int = 0) -> dict:
    keys = jax.random.split(jax.random.key(seed), 4)
    return {
        "users": draw_users(jax.random.fold_in(keys[3], 71), 0),
        "items": draw_items(jax.random.fold_in(keys[3], 71), 0),
        "pos_ids": place_ends(jax.random.randint(keys[2], (USERS,), 0, ITEMS), jax.random.fold_in(keys[2], 1), 0, ITEMS - 1).astype(jnp.int32),
    }


def reference(users, items, pos_ids):
    rows = users.shape[0]
    size = math.gcd(rows, 1024)
    count = rows // size
    bank = items.astype(jnp.float32)
    cols = jnp.arange(items.shape[0], dtype=jnp.int32)

    def step(carry, args):
        ublk, pblk = args
        user_block = ublk.astype(jnp.float32)
        logit = jnp.dot(user_block, bank.T, precision=lax.Precision.HIGHEST)
        mask = pblk[:, None] == cols[None, :]
        peak = jnp.max(logit, axis=1)
        total = jnp.sum(jnp.exp(logit - peak[:, None]), axis=1)
        lse = peak + jnp.log(total)
        positive = jnp.sum(jnp.where(mask, logit, jnp.float32(0.0)), axis=1)
        weights = (jnp.exp(logit - lse[:, None]) - mask.astype(jnp.float32)).astype(jnp.bfloat16)
        weight_full = weights.astype(jnp.float32)
        ugrad = jnp.dot(weight_full, bank, precision=lax.Precision.HIGHEST)
        carry = carry + jnp.dot(weight_full.T, user_block, precision=lax.Precision.HIGHEST)
        return carry, (lse - positive, ugrad)

    start = jnp.zeros(items.shape, jnp.float32)
    item_grad, outputs = lax.scan(step, start, (users.reshape(count, size, users.shape[1]), pos_ids.reshape(count, size)))
    loss = outputs[0].reshape(rows)
    user_grad = outputs[1].reshape(rows, users.shape[1])
    return (loss, user_grad, item_grad)
```

```python
import jax
import jax.numpy as jnp
from jax import lax
from jax.experimental import pallas as pl
from jax.experimental.pallas import tpu as pltpu
from jax.sharding import Mesh
from jax.sharding import PartitionSpec as P

AXES = ("xh", "z", "xl", "y", "c")
MESH = pl.DeviceIdType.MESH
F32 = jnp.float32
BF16 = jnp.bfloat16
NX, NY, NZ, NC = 4, 4, 8, 2
OWN = 40
ROW = 48
ITM = 256
E = 256
CH = NZ * ROW


def kernel(blk, items, loss_out, ug_out, ig_out, U, I, IT, HL, LG, EX, MB, SB, PB, W, ST, PT, YST, YPT, ZST, ZPT, SC,
           UG, YR2, YR1, ZR, G, PG, XR2, XR1,
           s_send, s_u, s_i, s_ys, s_yp, s_zs, s_zp, s_y2, s_y1, s_zr, s_pg, s_x2, s_x1):
    xh, z, xl, y, c = (lax.axis_index(a) for a in AXES)
    x = 2 * xh + xl

    def dev(dx=0, dy=0, dz=0, dc=0):
        nx = lax.rem(x + dx, NX)
        nc = lax.rem(c + dc, NC)
        return (nx // 2, lax.rem(z + dz, NZ), lax.rem(nx, 2), lax.rem(y + dy, NY), nc)

    sent = []

    def send(src, dst, recv, where):
        copy = pltpu.make_async_remote_copy(
            src_ref=src, dst_ref=dst, send_sem=s_send.at[len(sent)], recv_sem=recv,
            device_id=where, device_id_type=MESH,
        )
        copy.start()
        sent.append(copy)

    def arrived(dst, recv):
        pltpu.make_async_remote_copy(
            src_ref=dst, dst_ref=dst, send_sem=s_send.at[0], recv_sem=recv,
            device_id=dev(dc=1), device_id_type=MESH,
        ).wait_recv()

    yy = [lax.rem(y + d, NY) for d in range(NY)]
    zz = [lax.rem(z + d, NZ) for d in range(NZ)]
    xx = [lax.rem(x + d, NX) for d in range(NX)]
    co = 1 - c

    barrier = pltpu.get_barrier_semaphore()
    peers = [dict(dz=d) for d in range(1, NZ)] + [dict(dy=d) for d in range(1, NY)]
    peers += [dict(dx=1), dict(dx=3), dict(dc=1)]
    for p in peers:
        pl.semaphore_signal(barrier, inc=1, device_id=dev(**p), device_id_type=MESH)

    U[y * NZ + z] = blk[...]
    I[x * NC + c] = items[...]
    pl.semaphore_wait(barrier, len(peers))

    H = ITM // 2
    bo = x * NC + c

    def halves(b, order=(0, 1)):
        return [(h, I.at[b, pl.ds(h * H, H)], s_i.at[2 * b + h]) for h in order]

    mine = y * NZ + z
    for d in (1, 7, 2, 6, 3, 5, 4):
        send(blk, U.at[mine], s_u.at[mine], dev(dz=d))
    for d in (1, 3):
        send(blk, U.at[mine], s_u.at[mine], dev(dy=d))
    for dx, order in ((1, (0, 1)), (3, (1, 0))):
        for h, dst, sem in halves(bo, order):
            send(items.at[pl.ds(h * H, H)], dst, sem, dev(dx=dx))
    for h, dst, sem in halves(bo):
        send(items.at[pl.ds(h * H, H)], dst, sem, dev(dc=1))

    for d in (1, 7, 2, 6, 3, 5, 4):
        s = y * NZ + zz[d]
        arrived(U.at[s], s_u.at[s])
        for dy in (1, 3):
            send(U.at[s], U.at[s], s_u.at[s], dev(dy=dy))

    for dx, keep in ((3, 0), (1, 1)):
        b = xx[dx] * NC + c
        for h, ref, sem in halves(b, (keep, 1 - keep)):
            arrived(ref, sem)
            if h == keep:
                send(ref, ref, sem, dev(dx=4 - dx))
            send(ref, ref, sem, dev(dc=1))

    def place_ids(yi):
        part = U[pl.ds(yi * NZ, NZ), OWN:ROW, 0:128].astype(F32)
        n = lax.broadcasted_iota(jnp.int32, (128, CH), 1)
        k = (n * 1366) >> 16
        pick = jnp.where(n - k * ROW == lax.broadcasted_iota(jnp.int32, (128, CH), 0), 1.0, 0.0)
        pick = pick.astype(BF16)
        n8 = lax.broadcasted_iota(jnp.int32, (NZ, CH), 1)
        k8 = (n8 * 1366) >> 16
        here = k8 == lax.broadcasted_iota(jnp.int32, (NZ, CH), 0)
        for j in range(2):
            spread = jnp.dot(part[:, j, :].astype(BF16), pick, preferred_element_type=F32)
            HL[yi, j] = jnp.sum(jnp.where(here, spread, 0.0), axis=0, keepdims=True)

    n1 = lax.broadcasted_iota(jnp.int32, (1, CH), 1)
    valid = n1 - ((n1 * 1366) >> 16) * ROW < OWN

    def target(yi, bx, bc):
        owner = (bx // 2) * 128 + z * 16 + lax.rem(bx, 2) * 8 + y * 2 + bc
        match = (HL[yi, 0] == owner.astype(F32)) & valid
        return jnp.where(match, HL[yi, 1], -1.0)

    rows = lax.broadcasted_iota(jnp.int32, (ITM, 128), 0).astype(F32)

    def first(yi, bx, bc):
        b = bx * NC + bc
        users = U[pl.ds(yi * NZ, NZ)].reshape(CH, E)
        LG[...] = lax.dot_general(I[b], users, (((1,), (1,)), ((), ())), preferred_element_type=F32)
        at = target(yi, bx, bc)
        for j in range(CH // 128):
            cols = slice(128 * j, 128 * j + 128)
            lg = LG[:, cols]
            top = jnp.max(lg, axis=0, keepdims=True)
            ex = jnp.exp(lg - top)
            EX[b, yi, :, cols] = ex
            MB[yi, b, :, cols] = top
            SB[yi, b, :, cols] = jnp.sum(ex, axis=0, keepdims=True)
            PB[yi, b, :, cols] = jnp.sum(jnp.where(rows == at[:, cols], lg, 0.0), axis=0, keepdims=True)

    def turn(b):
        IT[b] = I[b].T

    place_ids(yy[0])
    for dx in (0, 3, 1):
        first(yy[0], xx[dx], c)
        turn(xx[dx] * NC + c)

    for dy, first_z in ((3, 0), (1, 1)):
        for d in range(NZ):
            s = yy[dy] * NZ + d
            arrived(U.at[s], s_u.at[s])
            if (d < NZ // 2) == (first_z == 0):
                send(U.at[s], U.at[s], s_u.at[s], dev(dy=4 - dy))

    b = xx[2] * NC + c
    for h, ref, sem in halves(b):
        arrived(ref, sem)
        send(ref, ref, sem, dev(dc=1))
    first(yy[0], xx[2], c)
    turn(b)
    for dx in (0, 3, 1, 2):
        b = xx[dx] * NC + co
        for h, ref, sem in halves(b):
            arrived(ref, sem)
        first(yy[0], xx[dx], co)
        turn(b)

    for dy in (3, 1):
        place_ids(yy[dy])
        lax.fori_loop(0, NX * NC, lambda i, _: (first(yy[dy], i // NC, lax.rem(i, NC)), 0)[1], 0)
    for d in range(NZ):
        s = yy[2] * NZ + d
        arrived(U.at[s], s_u.at[s])
    place_ids(yy[2])
    lax.fori_loop(0, NX * NC, lambda i, _: (first(yy[2], i // NC, lax.rem(i, NC)), 0)[1], 0)

    NR = CH // 128
    for k in range(NY):
        m = jnp.max(MB[k], axis=0)
        s = jnp.sum(SB[k] * jnp.exp(MB[k] - m[None]), axis=0)
        p = jnp.sum(PB[k], axis=0)
        for j in range(NR):
            cols = slice(128 * j, 128 * j + 128)
            r = NR * k + j
            ST[r : r + 1] = m[:, cols]
            ST[12 + r : 13 + r] = s[:, cols]
            PT[r : r + 1] = p[:, cols]
    PT[12:16] = jnp.zeros((4, 128), F32)

    def combine(parts):
        m = parts[0][0:12]
        for q in parts[1:]:
            m = jnp.maximum(m, q[0:12])
        s = jnp.zeros_like(m)
        for q in parts:
            s = s + q[12:24] * jnp.exp(q[0:12] - m)
        return m, s

    for d in (1, 3, 2):
        send(ST, YST.at[y], s_ys.at[y], dev(dy=d))
    for d in (1, 3, 2):
        send(PT, YPT.at[y], s_yp.at[y], dev(dy=d))
    for d in (1, 3, 2):
        arrived(YST.at[yy[d]], s_ys.at[yy[d]])
    YST[y] = ST[...]
    m, s = combine([YST[k] for k in range(NY)])
    ZST[z, 0:12] = m
    ZST[z, 12:24] = s
    for d in (4, 3, 5, 2, 6, 1, 7):
        send(ZST.at[z], ZST.at[z], s_zs.at[z], dev(dz=d))
    for d in (1, 3, 2):
        arrived(YPT.at[yy[d]], s_yp.at[yy[d]])
    YPT[y] = PT[...]
    ZPT[z] = (YPT[0] + YPT[1]) + (YPT[2] + YPT[3])
    for d in (4, 3, 5, 2, 6, 1, 7):
        send(ZPT.at[z], ZPT.at[z], s_zp.at[z], dev(dz=d))
    for d in (1, 7, 2, 6, 3, 5, 4):
        arrived(ZST.at[zz[d]], s_zs.at[zz[d]])
    m, s = combine([ZST[k] for k in range(NZ)])
    lse = m + jnp.log(s)
    for k in range(NY):
        for j in range(NR):
            r = NR * k + j
            SC[k, :, 128 * j : 128 * j + 128] = lse[r : r + 1]

    def second(yi, bx, bc):
        b = bx * NC + bc
        at = target(yi, bx, bc)
        scale = jnp.where(valid, jnp.exp(MB[yi, b] - SC[yi]), 0.0)
        for j in range(CH // 128):
            cols = slice(128 * j, 128 * j + 128)
            w = EX[b, yi, :, cols] * scale[:, cols]
            w = w - jnp.where(rows == at[:, cols], 1.0, 0.0)
            W[b, yi, :, cols] = w.astype(BF16)

    def user_terms(d):
        yi = yy[d]
        lax.fori_loop(0, NX * NC, lambda i, _: (second(yi, i // NC, lax.rem(i, NC)), 0)[1], 0)
        acc = jnp.dot(IT[0], W[0, yi], preferred_element_type=F32)
        for b in range(1, NX * NC):
            acc += jnp.dot(IT[b], W[b, yi], preferred_element_type=F32)
        UG[d] = acc.T.reshape(NZ, ROW, E)

    HZ = NZ // 2
    user_terms(2)
    lo, hi = pl.ds(0, HZ), pl.ds(HZ, HZ)
    own = pl.ds(0, OWN)
    send(UG.at[2, lo, own], YR2.at[0], s_y2.at[0], dev(dy=1))
    send(UG.at[2, hi, own], YR2.at[1], s_y2.at[1], dev(dy=3))
    user_terms(1)
    send(UG.at[1, hi, own], YR1.at[0, hi], s_y1.at[1], dev(dy=1))
    user_terms(3)
    send(UG.at[3, lo, own], YR1.at[1, lo], s_y1.at[2], dev(dy=3))
    user_terms(0)

    def item_terms(b):
        acc = jnp.dot(W[b, 0], U[0:NZ].reshape(CH, E), preferred_element_type=F32)
        for k in range(1, NY):
            acc += jnp.dot(W[b, k], U[k * NZ : k * NZ + NZ].reshape(CH, E), preferred_element_type=F32)
        G[b] = acc

    for dx in (2, 1):
        b = xx[dx] * NC + co
        item_terms(b)
        send(G.at[b], PG.at[xx[dx]], s_pg.at[xx[dx]], dev(dc=1))
    arrived(YR2.at[0], s_y2.at[0])
    UG[1, 0:HZ, 0:OWN] += YR2[0]
    send(UG.at[1, lo, own], YR1.at[0, lo], s_y1.at[0], dev(dy=1))
    arrived(YR2.at[1], s_y2.at[1])
    UG[3, HZ:NZ, 0:OWN] += YR2[1]
    send(UG.at[3, hi, own], YR1.at[1, hi], s_y1.at[3], dev(dy=3))
    for dx in (3, 0):
        b = xx[dx] * NC + co
        item_terms(b)
        send(G.at[b], PG.at[xx[dx]], s_pg.at[xx[dx]], dev(dc=1))

    def own_terms(dx):
        b = xx[dx] * NC + c
        item_terms(b)
        arrived(PG.at[xx[dx]], s_pg.at[xx[dx]])
        G[b] += PG[xx[dx]]
        return b

    top, bot = pl.ds(0, H), pl.ds(H, H)
    b = own_terms(2)
    send(G.at[b, top], XR2.at[0], s_x2.at[0], dev(dx=1))
    send(G.at[b, bot], XR2.at[1], s_x2.at[1], dev(dx=3))
    b1 = own_terms(1)
    send(G.at[b1, bot], XR1.at[0, bot], s_x1.at[1], dev(dx=1))
    b3 = own_terms(3)
    send(G.at[b3, top], XR1.at[1, top], s_x1.at[2], dev(dx=3))

    for i, part in ((1, hi), (2, lo), (0, lo), (3, hi)):
        arrived(YR1.at[i // 2, part], s_y1.at[i])
    UG[0, :, 0:OWN] = UG[0, :, 0:OWN] + YR1[0] + YR1[1]
    for d in (4, 3, 5, 2, 6, 1, 7):
        send(UG.at[0, zz[d], own], ZR.at[z], s_zr.at[z], dev(dz=d))

    b0 = own_terms(0)
    arrived(XR2.at[0], s_x2.at[0])
    G[b1, 0:H] += XR2[0]
    send(G.at[b1, top], XR1.at[0, top], s_x1.at[0], dev(dx=1))
    arrived(XR2.at[1], s_x2.at[1])
    G[b3, H:ITM] += XR2[1]
    send(G.at[b3, bot], XR1.at[1, bot], s_x1.at[3], dev(dx=3))

    for d in (1, 7, 2, 6, 3, 5, 4):
        arrived(ZPT.at[zz[d]], s_zp.at[zz[d]])
    pos = ZPT[0]
    for k in range(1, NZ):
        pos = pos + ZPT[k]
    for k in range(NY):
        for j in range(NR):
            r = NR * k + j
            PB[k, 0, :, 128 * j : 128 * j + 128] = lse[r : r + 1] - pos[r : r + 1]
    line = PB[y, 0]
    out = line[:, 0:ROW]
    for k in range(1, NZ):
        out = jnp.where(z == k, line[:, ROW * k : ROW * k + ROW], out)
    loss_out[:, 0:ROW] = out
    loss_out[:, ROW:128] = jnp.zeros((1, 128 - ROW), F32)

    total = UG[0, z, 0:OWN]
    for d in range(1, NZ):
        arrived(ZR.at[zz[d]], s_zr.at[zz[d]])
        total = total + ZR[zz[d]]
    ug_out[...] = total

    for i, part in ((1, bot), (2, top), (0, top), (3, bot)):
        arrived(XR1.at[i // 2, part], s_x1.at[i])
    ig_out[...] = G[b0] + XR1[0] + XR1[1]

    for copy in sent:
        copy.wait_send()


def local(users, items, pos_ids):
    ids = jnp.stack([pos_ids >> 8, pos_ids & 255]).astype(BF16)
    ids = jnp.pad(ids, ((0, ROW - OWN - 2), (0, E - OWN)))
    blk = jnp.concatenate([users, ids], axis=0)
    V = pltpu.VMEM
    D = pltpu.SemaphoreType.DMA
    scratch = [
        V((NY * NZ, ROW, E), BF16),
        V((NX * NC, ITM, E), BF16),
        V((NX * NC, E, ITM), BF16),
        V((NY, 2, 1, CH), F32),
        V((ITM, CH), F32),
        V((NX * NC, NY, ITM, CH), F32),
        V((NY, NX * NC, 1, CH), F32),
        V((NY, NX * NC, 1, CH), F32),
        V((NY, NX * NC, 1, CH), F32),
        V((NX * NC, NY, ITM, CH), BF16),
        V((24, 128), F32),
        V((16, 128), F32),
        V((NY, 24, 128), F32),
        V((NY, 16, 128), F32),
        V((NZ, 24, 128), F32),
        V((NZ, 16, 128), F32),
        V((NY, 1, CH), F32),
        V((NY, NZ, ROW, E), F32),
        V((2, NZ // 2, OWN, E), F32),
        V((2, NZ, OWN, E), F32),
        V((NZ, OWN, E), F32),
        V((NX * NC, ITM, E), F32),
        V((NX, ITM, E), F32),
        V((2, ITM // 2, E), F32),
        V((2, ITM, E), F32),
        D((128,)),
        D((NY * NZ,)),
        D((2 * NX * NC,)),
        D((NY,)), D((NY,)), D((NZ,)), D((NZ,)),
        D((2,)), D((4,)), D((NZ,)), D((NX,)), D((2,)), D((4,)),
    ]
    loss, ug, ig = pl.pallas_call(
        kernel,
        out_shape=(
            jax.ShapeDtypeStruct((1, 128), F32),
            jax.ShapeDtypeStruct((OWN, E), F32),
            jax.ShapeDtypeStruct((ITM, E), F32),
        ),
        in_specs=[pl.BlockSpec(memory_space=pltpu.VMEM)] * 2,
        out_specs=tuple([pl.BlockSpec(memory_space=pltpu.VMEM)] * 3),
        scratch_shapes=scratch,
        compiler_params=pltpu.CompilerParams(
            collective_id=0, has_side_effects=True, vmem_limit_bytes=60 * 2**20
        ),
        name="infonce",
    )(blk, items)
    return loss[0, :OWN], ug, ig


def solution(mesh):
    torus = Mesh(mesh.devices.reshape(2, NZ, 2, NY, NC), AXES)
    every = P(AXES)
    return jax.shard_map(
        local,
        mesh=torus,
        in_specs=(P(AXES, None), P(AXES, None), every),
        out_specs=(every, P(AXES, None), P(AXES, None)),
        check_vma=False,
    )
```

```python
import jax
import jax.numpy as jnp
from jax import lax
from jax.experimental import pallas as pl
from jax.experimental.pallas import tpu as pltpu
from jax.sharding import Mesh
from jax.sharding import PartitionSpec as P

AXES = ("xh", "z", "xl", "y", "c")
MESH = pl.DeviceIdType.MESH
F32 = jnp.float32
BF16 = jnp.bfloat16
NX, NY, NZ, NC = 4, 4, 8, 2
OWN = 40
ROW = 48
ITM = 256
E = 256
CH = NZ * ROW


TOP = 32704.0


def code(v, q, m):
    for j in range(v.shape[1] // 128):
        cols = slice(128 * j, 128 * j + 128)
        part = v[:, cols]
        most = jnp.maximum(jnp.max(jnp.abs(part), axis=0, keepdims=True), 1e-30)
        m[:, cols] = most
        q[:, cols] = jnp.round(part * (TOP / most)).astype(jnp.int16)


def decode(q, m):
    return q.astype(F32) * (m * (1.0 / TOP))


def kernel(users, items, ids, loss_out, ug_out, ig_out, U, I, ID, IT, UT, HL, LG, EX, MB, SB, PB, W, ST, PT, YST, YPT, ZST, ZPT,
           SC, UG, UZ, QY2, MY2, QY1, MY1, YQ2, YM2, YQ1, YM1, QZ, MZ, ZQ, ZM, G, QP, MP, PQ, PM, QX2, MX2, QX1, MX1, XQ2, XM2,
           XQ1, XM1, s_in, s_send, s_u, s_i, s_ys, s_yp, s_zs, s_zp, s_y2, s_y1, s_zr, s_pg, s_x2, s_x1):
    xh, z, xl, y, c = (lax.axis_index(a) for a in AXES)
    x = 2 * xh + xl

    def dev(dx=0, dy=0, dz=0, dc=0):
        nx = lax.rem(x + dx, NX)
        nc = lax.rem(c + dc, NC)
        return (nx // 2, lax.rem(z + dz, NZ), lax.rem(nx, 2), lax.rem(y + dy, NY), nc)

    sent = []

    def send(src, dst, recv, where):
        copy = pltpu.make_async_remote_copy(
            src_ref=src, dst_ref=dst, send_sem=s_send.at[len(sent)], recv_sem=recv,
            device_id=where, device_id_type=MESH,
        )
        copy.start()
        sent.append(copy)

    def arrived(dst, recv):
        pltpu.make_async_remote_copy(
            src_ref=dst, dst_ref=dst, send_sem=s_send.at[0], recv_sem=recv,
            device_id=dev(dc=1), device_id_type=MESH,
        ).wait_recv()

    yy = [lax.rem(y + d, NY) for d in range(NY)]
    zz = [lax.rem(z + d, NZ) for d in range(NZ)]
    xx = [lax.rem(x + d, NX) for d in range(NX)]
    co = 1 - c

    mine = y * NZ + z
    bo = x * NC + c
    inputs = [
        pltpu.make_async_copy(users, U.at[mine, pl.ds(0, OWN)], s_in.at[0]),
        pltpu.make_async_copy(items, I.at[bo], s_in.at[1]),
        pltpu.make_async_copy(ids, ID, s_in.at[2]),
    ]
    for copy in inputs:
        copy.start()
    barrier = pltpu.get_barrier_semaphore()
    peers = [dict(dz=d) for d in range(1, NZ)] + [dict(dy=d) for d in range(1, NY)]
    peers += [dict(dx=1), dict(dx=3), dict(dc=1)]
    for p in peers:
        pl.semaphore_signal(barrier, inc=1, device_id=dev(**p), device_id_type=MESH)

    for copy in inputs:
        copy.wait()
    PB[0, 0] = jnp.zeros((1, CH), F32)
    PB[1, 0] = jnp.zeros((1, CH), F32)
    PB[0, 0, :, 0:OWN] = (ID[...] >> 8).astype(F32)
    PB[1, 0, :, 0:OWN] = (ID[...] & 255).astype(F32)
    r8 = lax.broadcasted_iota(jnp.int32, (ROW - OWN, E), 0)
    pad = jnp.where(r8 == 0, PB[0, 0, :, 0:E], jnp.where(r8 == 1, PB[1, 0, :, 0:E], 0.0))
    U[mine, OWN:ROW] = pad.astype(BF16)
    pl.semaphore_wait(barrier, len(peers))

    H = ITM // 2

    def halves(b, order=(0, 1)):
        return [(h, I.at[b, pl.ds(h * H, H)], s_i.at[2 * b + h]) for h in order]

    for d in (1, 7, 2, 6, 3, 5, 4):
        send(U.at[mine], U.at[mine], s_u.at[mine], dev(dz=d))
    for d in (1, 3):
        send(U.at[mine], U.at[mine], s_u.at[mine], dev(dy=d))
    for dx, order in ((1, (0, 1)), (3, (1, 0))):
        for h, dst, sem in halves(bo, order):
            send(dst, dst, sem, dev(dx=dx))
    for h, dst, sem in halves(bo):
        send(dst, dst, sem, dev(dc=1))

    for d in (1, 7, 2, 6, 3, 5, 4):
        s = y * NZ + zz[d]
        arrived(U.at[s], s_u.at[s])
        for dy in (1, 3):
            send(U.at[s], U.at[s], s_u.at[s], dev(dy=dy))

    for dx, keep in ((3, 0), (1, 1)):
        b = xx[dx] * NC + c
        for h, ref, sem in halves(b, (keep, 1 - keep)):
            arrived(ref, sem)
            if h == keep:
                send(ref, ref, sem, dev(dx=4 - dx))
            send(ref, ref, sem, dev(dc=1))

    def place_ids(yi):
        UT[yi] = U[pl.ds(yi * NZ, NZ)].reshape(CH, E).T
        part = U[pl.ds(yi * NZ, NZ), OWN:ROW, 0:128].astype(F32)
        n = lax.broadcasted_iota(jnp.int32, (128, CH), 1)
        k = (n * 1366) >> 16
        pick = jnp.where(n - k * ROW == lax.broadcasted_iota(jnp.int32, (128, CH), 0), 1.0, 0.0)
        pick = pick.astype(BF16)
        n8 = lax.broadcasted_iota(jnp.int32, (NZ, CH), 1)
        k8 = (n8 * 1366) >> 16
        here = k8 == lax.broadcasted_iota(jnp.int32, (NZ, CH), 0)
        for j in range(2):
            spread = jnp.dot(part[:, j, :].astype(BF16), pick, preferred_element_type=F32)
            HL[yi, j] = jnp.sum(jnp.where(here, spread, 0.0), axis=0, keepdims=True)

    n1 = lax.broadcasted_iota(jnp.int32, (1, CH), 1)
    valid = n1 - ((n1 * 1366) >> 16) * ROW < OWN

    def target(yi, bx, bc):
        owner = (bx // 2) * 128 + z * 16 + lax.rem(bx, 2) * 8 + y * 2 + bc
        match = (HL[yi, 0] == owner.astype(F32)) & valid
        return jnp.where(match, HL[yi, 1], -1.0)

    rows = lax.broadcasted_iota(jnp.int32, (ITM, 128), 0).astype(F32)

    def first(yi, bx, bc):
        b = bx * NC + bc
        LG[...] = jnp.dot(I[b], UT[yi], preferred_element_type=F32)
        at = target(yi, bx, bc)
        for j in range(CH // 128):
            cols = slice(128 * j, 128 * j + 128)
            lg = LG[:, cols]
            top = jnp.max(lg, axis=0, keepdims=True)
            ex = jnp.exp(lg - top)
            EX[b, yi, :, cols] = ex
            MB[yi, b, :, cols] = top
            SB[yi, b, :, cols] = jnp.sum(ex, axis=0, keepdims=True)
            PB[yi, b, :, cols] = jnp.sum(jnp.where(rows == at[:, cols], lg, 0.0), axis=0, keepdims=True)

    def turn(b):
        IT[b] = I[b].T

    place_ids(yy[0])
    for dx in (0, 3, 1):
        first(yy[0], xx[dx], c)
        turn(xx[dx] * NC + c)

    for dy, first_z in ((3, 0), (1, 1)):
        for d in range(NZ):
            s = yy[dy] * NZ + d
            arrived(U.at[s], s_u.at[s])
            if (d < NZ // 2) == (first_z == 0):
                send(U.at[s], U.at[s], s_u.at[s], dev(dy=4 - dy))

    b = xx[2] * NC + c
    for h, ref, sem in halves(b):
        arrived(ref, sem)
        send(ref, ref, sem, dev(dc=1))
    first(yy[0], xx[2], c)
    turn(b)
    for dx in (0, 3, 1, 2):
        b = xx[dx] * NC + co
        for h, ref, sem in halves(b):
            arrived(ref, sem)
        first(yy[0], xx[dx], co)
        turn(b)

    for dy in (3, 1):
        place_ids(yy[dy])
        lax.fori_loop(0, NX * NC, lambda i, _: (first(yy[dy], i // NC, lax.rem(i, NC)), 0)[1], 0)
    for d in range(NZ):
        s = yy[2] * NZ + d
        arrived(U.at[s], s_u.at[s])
    place_ids(yy[2])
    lax.fori_loop(0, NX * NC, lambda i, _: (first(yy[2], i // NC, lax.rem(i, NC)), 0)[1], 0)

    NR = CH // 128
    for k in range(NY):
        m = jnp.max(MB[k], axis=0)
        s = jnp.sum(SB[k] * jnp.exp(MB[k] - m[None]), axis=0)
        p = jnp.sum(PB[k], axis=0)
        for j in range(NR):
            cols = slice(128 * j, 128 * j + 128)
            r = NR * k + j
            ST[r : r + 1] = m[:, cols]
            ST[12 + r : 13 + r] = s[:, cols]
            PT[r : r + 1] = p[:, cols]
    PT[12:16] = jnp.zeros((4, 128), F32)

    def combine(parts):
        m = parts[0][0:12]
        for q in parts[1:]:
            m = jnp.maximum(m, q[0:12])
        s = jnp.zeros_like(m)
        for q in parts:
            s = s + q[12:24] * jnp.exp(q[0:12] - m)
        return m, s

    for d in (1, 3, 2):
        send(ST, YST.at[y], s_ys.at[y], dev(dy=d))
    for d in (1, 3, 2):
        send(PT, YPT.at[y], s_yp.at[y], dev(dy=d))
    for d in (1, 3, 2):
        arrived(YST.at[yy[d]], s_ys.at[yy[d]])
    YST[y] = ST[...]
    m, s = combine([YST[k] for k in range(NY)])
    ZST[z, 0:12] = m
    ZST[z, 12:24] = s
    for d in (4, 3, 5, 2, 6, 1, 7):
        send(ZST.at[z], ZST.at[z], s_zs.at[z], dev(dz=d))
    for d in (1, 3, 2):
        arrived(YPT.at[yy[d]], s_yp.at[yy[d]])
    YPT[y] = PT[...]
    ZPT[z] = (YPT[0] + YPT[1]) + (YPT[2] + YPT[3])
    for d in (4, 3, 5, 2, 6, 1, 7):
        send(ZPT.at[z], ZPT.at[z], s_zp.at[z], dev(dz=d))
    for d in (1, 7, 2, 6, 3, 5, 4):
        arrived(ZST.at[zz[d]], s_zs.at[zz[d]])
    m, s = combine([ZST[k] for k in range(NZ)])
    lse = m + jnp.log(s)
    for k in range(NY):
        for j in range(NR):
            r = NR * k + j
            SC[k, :, 128 * j : 128 * j + 128] = lse[r : r + 1]

    def second(yi, bx, bc):
        b = bx * NC + bc
        at = target(yi, bx, bc)
        scale = jnp.where(valid, jnp.exp(MB[yi, b] - SC[yi]), 0.0)
        for j in range(CH // 128):
            cols = slice(128 * j, 128 * j + 128)
            w = EX[b, yi, :, cols] * scale[:, cols]
            w = w - jnp.where(rows == at[:, cols], 1.0, 0.0)
            W[b, yi, :, cols] = w.astype(BF16)

    def user_terms(d):
        yi = yy[d]
        lax.fori_loop(0, NX * NC, lambda i, _: (second(yi, i // NC, lax.rem(i, NC)), 0)[1], 0)
        acc = jnp.dot(IT[0], W[0, yi], preferred_element_type=F32)
        for b in range(1, NX * NC):
            acc += jnp.dot(IT[b], W[b, yi], preferred_element_type=F32)
        UG[d] = acc

    H = E // 2
    half = [pl.ds(0, H), pl.ds(H, H)]

    def send2(q, qto, m, mto, recv, i, where):
        send(q, qto, recv.at[i, 0], where)
        send(m, mto, recv.at[i, 1], where)

    def arrived2(q, m, recv, i):
        arrived(q, recv.at[i, 0])
        arrived(m, recv.at[i, 1])

    user_terms(2)
    for i in range(2):
        code(UG[2, H * i : H * i + H], QY2.at[i], MY2.at[i])
        send2(QY2.at[i], YQ2.at[i], MY2.at[i], YM2.at[i], s_y2, i, dev(dy=1 + 2 * i))

    def direct(d, i):
        h = 1 - i
        k = 2 * i + h
        code(UG[d, H * h : H * h + H], QY1.at[k], MY1.at[k])
        send2(QY1.at[k], YQ1.at[k], MY1.at[k], YM1.at[k], s_y1, k, dev(dy=d))

    def relayed(d, i):
        h = i
        k = 2 * i + h
        arrived2(YQ2.at[i], YM2.at[i], s_y2, i)
        code(UG[d, H * h : H * h + H] + decode(YQ2[i], YM2[i]), QY1.at[k], MY1.at[k])
        send2(QY1.at[k], YQ1.at[k], MY1.at[k], YM1.at[k], s_y1, k, dev(dy=d))

    user_terms(1)
    direct(1, 0)
    user_terms(3)
    direct(3, 1)
    relayed(1, 0)
    relayed(3, 1)
    user_terms(0)

    def item_terms(b):
        acc = jnp.dot(W[b, 0], U[0:NZ].reshape(CH, E), preferred_element_type=F32)
        for k in range(1, NY):
            acc += jnp.dot(W[b, k], U[k * NZ : k * NZ + NZ].reshape(CH, E), preferred_element_type=F32)
        G[b] = acc

    for dx in (2, 1, 3, 0):
        b = xx[dx] * NC + co
        item_terms(b)
        code(G[b], QP.at[dx], MP.at[dx])
        send2(QP.at[dx], PQ.at[dx], MP.at[dx], PM.at[dx], s_pg, dx, dev(dc=1))

    total = []
    for h in range(2):
        v = UG[0, H * h : H * h + H]
        for i in range(2):
            k = 2 * i + h
            arrived2(YQ1.at[k], YM1.at[k], s_y1, k)
            v = v + decode(YQ1[k], YM1[k])
        UG[0, H * h : H * h + H] = v
    UZ[...] = UG[0].T.reshape(NZ, ROW, E)
    for d in (4, 3, 5, 2, 6, 1, 7):
        code(UZ[zz[d], 0:OWN], QZ.at[d], MZ.at[d])
        send2(QZ.at[d], ZQ.at[d], MZ.at[d], ZM.at[d], s_zr, d, dev(dz=d))

    def own_terms(dx):
        b = xx[dx] * NC + c
        item_terms(b)
        arrived2(PQ.at[dx], PM.at[dx], s_pg, dx)
        G[b] += decode(PQ[dx], PM[dx])
        return b

    b2 = own_terms(2)
    for i in range(2):
        code(G[b2, H * i : H * i + H], QX2.at[i], MX2.at[i])
        send2(QX2.at[i], XQ2.at[i], MX2.at[i], XM2.at[i], s_x2, i, dev(dx=1 + 2 * i))

    def x_direct(dx, i):
        b = own_terms(dx)
        h = 1 - i
        k = 2 * i + h
        code(G[b, H * h : H * h + H], QX1.at[k], MX1.at[k])
        send2(QX1.at[k], XQ1.at[k], MX1.at[k], XM1.at[k], s_x1, k, dev(dx=dx))
        return b

    def x_relayed(b, dx, i):
        h = i
        k = 2 * i + h
        arrived2(XQ2.at[i], XM2.at[i], s_x2, i)
        code(G[b, H * h : H * h + H] + decode(XQ2[i], XM2[i]), QX1.at[k], MX1.at[k])
        send2(QX1.at[k], XQ1.at[k], MX1.at[k], XM1.at[k], s_x1, k, dev(dx=dx))

    b1 = x_direct(1, 0)
    b3 = x_direct(3, 1)
    x_relayed(b1, 1, 0)
    x_relayed(b3, 3, 1)
    b0 = own_terms(0)

    for d in (1, 7, 2, 6, 3, 5, 4):
        arrived(ZPT.at[zz[d]], s_zp.at[zz[d]])
    pos = ZPT[0]
    for k in range(1, NZ):
        pos = pos + ZPT[k]
    for k in range(NY):
        for j in range(NR):
            r = NR * k + j
            PB[k, 0, :, 128 * j : 128 * j + 128] = lse[r : r + 1] - pos[r : r + 1]
    line = PB[y, 0]
    out = line[:, 0:ROW]
    for k in range(1, NZ):
        out = jnp.where(z == k, line[:, ROW * k : ROW * k + ROW], out)
    loss_out[:, 0:ROW] = out
    loss_out[:, ROW:128] = jnp.zeros((1, 128 - ROW), F32)

    total = UZ[z, 0:OWN]
    for d in (1, 7, 2, 6, 3, 5, 4):
        arrived2(ZQ.at[d], ZM.at[d], s_zr, d)
        total = total + decode(ZQ[d], ZM[d])
    ug_out[...] = total

    for h in range(2):
        v = G[b0, H * h : H * h + H]
        for i in range(2):
            k = 2 * i + h
            arrived2(XQ1.at[k], XM1.at[k], s_x1, k)
            v = v + decode(XQ1[k], XM1[k])
        ig_out[H * h : H * h + H] = v

    for copy in sent:
        copy.wait_send()


def finish(loss, ug, ig, loss_out, ug_out, ig_out, vl, vu, vi, sem):
    into = [
        pltpu.make_async_copy(a, b, sem.at[k])
        for k, (a, b) in enumerate(((ig, vi), (ug, vu), (loss, vl)))
    ]
    out = [
        pltpu.make_async_copy(a, b, sem.at[k + 3])
        for k, (a, b) in enumerate(((vi, ig_out), (vu, ug_out), (vl, loss_out)))
    ]
    for copy in into:
        copy.start()
    for a, b in zip(into, out):
        a.wait()
        b.start()
    for copy in out:
        copy.wait()


def local(users, items, pos_ids):
    V = pltpu.VMEM
    D = pltpu.SemaphoreType.DMA
    I16 = jnp.int16
    HE = E // 2
    scratch = [
        V((NY * NZ, ROW, E), BF16),
        V((NX * NC, ITM, E), BF16),
        V((1, OWN), jnp.int32),
        V((NX * NC, E, ITM), BF16),
        V((NY, E, CH), BF16),
        V((NY, 2, 1, CH), F32),
        V((ITM, CH), F32),
        V((NX * NC, NY, ITM, CH), F32),
        V((NY, NX * NC, 1, CH), F32),
        V((NY, NX * NC, 1, CH), F32),
        V((NY, NX * NC, 1, CH), F32),
        V((NX * NC, NY, ITM, CH), BF16),
        V((24, 128), F32),
        V((16, 128), F32),
        V((NY, 24, 128), F32),
        V((NY, 16, 128), F32),
        V((NZ, 24, 128), F32),
        V((NZ, 16, 128), F32),
        V((NY, 1, CH), F32),
        V((NY, E, CH), F32),
        V((NZ, ROW, E), F32),
        V((2, HE, CH), I16), V((2, 1, CH), F32),
        V((4, HE, CH), I16), V((4, 1, CH), F32),
        V((2, HE, CH), I16), V((2, 1, CH), F32),
        V((4, HE, CH), I16), V((4, 1, CH), F32),
        V((NZ, OWN, E), I16), V((NZ, 1, E), F32),
        V((NZ, OWN, E), I16), V((NZ, 1, E), F32),
        V((NX * NC, ITM, E), F32),
        V((NX, ITM, E), I16), V((NX, 1, E), F32),
        V((NX, ITM, E), I16), V((NX, 1, E), F32),
        V((2, HE, E), I16), V((2, 1, E), F32),
        V((4, HE, E), I16), V((4, 1, E), F32),
        V((2, HE, E), I16), V((2, 1, E), F32),
        V((4, HE, E), I16), V((4, 1, E), F32),
        D((3,)),
        D((144,)),
        D((NY * NZ,)),
        D((2 * NX * NC,)),
        D((NY,)), D((NY,)), D((NZ,)), D((NZ,)),
        D((2, 2)), D((4, 2)), D((NZ, 2)), D((NX, 2)), D((2, 2)), D((4, 2)),
    ]
    outs = (
        jax.ShapeDtypeStruct((1, 128), F32),
        jax.ShapeDtypeStruct((OWN, E), F32),
        jax.ShapeDtypeStruct((ITM, E), F32),
    )
    hbm = pl.BlockSpec(memory_space=pl.ANY)
    loss, ug, ig = pl.pallas_call(
        kernel,
        out_shape=outs,
        in_specs=[hbm] * 3,
        out_specs=tuple([pl.BlockSpec(memory_space=pltpu.VMEM)] * 3),
        scratch_shapes=scratch,
        compiler_params=pltpu.CompilerParams(
            collective_id=0, has_side_effects=True, vmem_limit_bytes=60 * 2**20
        ),
        name="infonce",
    )(users, items, pos_ids.reshape(1, OWN))
    loss, ug, ig = pl.pallas_call(
        finish,
        out_shape=outs,
        in_specs=[hbm] * 3,
        out_specs=tuple([hbm] * 3),
        scratch_shapes=[V(o.shape, o.dtype) for o in outs] + [D((6,))],
        name="finish",
    )(loss, ug, ig)
    return loss[0, :OWN], ug, ig


def solution(mesh):
    torus = Mesh(mesh.devices.reshape(2, NZ, 2, NY, NC), AXES)
    every = P(AXES)
    return jax.shard_map(
        local,
        mesh=torus,
        in_specs=(P(AXES, None), P(AXES, None), every),
        out_specs=(every, P(AXES, None), P(AXES, None)),
        check_vma=False,
    )
```

```python
import jax
import jax.numpy as jnp
from jax import lax
from jax.experimental import pallas as pl
from jax.experimental.pallas import tpu as pltpu
from jax.sharding import Mesh
from jax.sharding import PartitionSpec as P

AXES = ("xh", "z", "xl", "y", "c")
MESH = pl.DeviceIdType.MESH
F32 = jnp.float32
BF16 = jnp.bfloat16
NX, NY, NZ, NC = 4, 4, 8, 2
OWN = 40
ROW = 48
ITM = 256
E = 256
CH = NZ * ROW


TOP = 32704.0


def code(v, q, m):
    for j in range(v.shape[1] // 128):
        cols = slice(128 * j, 128 * j + 128)
        part = v[:, cols]
        most = jnp.maximum(jnp.max(jnp.abs(part), axis=0, keepdims=True), 1e-30)
        m[:, cols] = most
        q[:, cols] = jnp.round(part * (TOP / most)).astype(jnp.int16)


def decode(q, m):
    return q.astype(F32) * (m * (1.0 / TOP))


def kernel(users, items, ids, loss_out, ug_out, ig_out, U, I, ID, IT, UT, HL, LGA, LGB, EX, MB, SB, PB, W, ST, PT, YST, YPT, ZST, ZPT,
           SC, UG, UZ, QY2, MY2, QY1, MY1, YQ2, YM2, YQ1, YM1, QZ, MZ, ZQ, ZM, G, QP, MP, PQ, PM, QX2, MX2, QX1, MX1, XQ2, XM2,
           XQ1, XM1, OL, OU, OI, s_in, s_out, s_send, s_u, s_i, s_ys, s_yp, s_zs, s_zp, s_y2, s_y1, s_zr, s_pg, s_x2, s_x1):
    xh, z, xl, y, c = (lax.axis_index(a) for a in AXES)
    x = 2 * xh + xl

    def dev(dx=0, dy=0, dz=0, dc=0):
        nx = lax.rem(x + dx, NX)
        nc = lax.rem(c + dc, NC)
        return (nx // 2, lax.rem(z + dz, NZ), lax.rem(nx, 2), lax.rem(y + dy, NY), nc)

    sent = []

    def send(src, dst, recv, where):
        copy = pltpu.make_async_remote_copy(
            src_ref=src, dst_ref=dst, send_sem=s_send.at[0], recv_sem=recv,
            device_id=where, device_id_type=MESH,
        )
        copy.start()
        sent.append(copy)

    stored = []

    def store(src, dst, i):
        copy = pltpu.make_async_copy(src, dst, s_out.at[i])
        copy.start()
        stored.append(copy)

    def arrived(dst, recv):
        pltpu.make_async_remote_copy(
            src_ref=dst, dst_ref=dst, send_sem=s_send.at[0], recv_sem=recv,
            device_id=dev(dc=1), device_id_type=MESH,
        ).wait_recv()

    yy = [lax.rem(y + d, NY) for d in range(NY)]
    zz = [lax.rem(z + d, NZ) for d in range(NZ)]
    xx = [lax.rem(x + d, NX) for d in range(NX)]
    co = 1 - c

    mine = y * NZ + z
    bo = c * NX + x
    inputs = [
        pltpu.make_async_copy(users, U.at[mine, pl.ds(0, OWN)], s_in.at[0]),
        pltpu.make_async_copy(items, I.at[bo], s_in.at[1]),
        pltpu.make_async_copy(ids, ID, s_in.at[2]),
    ]
    for copy in inputs:
        copy.start()
    barrier = pltpu.get_barrier_semaphore()
    peers = [dict(dz=d) for d in range(1, NZ)] + [dict(dy=d) for d in range(1, NY)]
    peers += [dict(dx=1), dict(dx=3), dict(dc=1)]
    for p in peers:
        pl.semaphore_signal(barrier, inc=1, device_id=dev(**p), device_id_type=MESH)

    for copy in inputs:
        copy.wait()
    PB[0, 0] = jnp.zeros((1, CH), F32)
    PB[1, 0] = jnp.zeros((1, CH), F32)
    PB[0, 0, :, 0:OWN] = (ID[...] >> 8).astype(F32)
    PB[1, 0, :, 0:OWN] = (ID[...] & 255).astype(F32)
    r8 = lax.broadcasted_iota(jnp.int32, (ROW - OWN, E), 0)
    pad = jnp.where(r8 == 0, PB[0, 0, :, 0:E], jnp.where(r8 == 1, PB[1, 0, :, 0:E], 0.0))
    U[mine, OWN:ROW] = pad.astype(BF16)
    pl.semaphore_wait(barrier, len(peers))

    H = ITM // 2

    def halves(b, order=(0, 1)):
        return [(h, I.at[b, pl.ds(h * H, H)], s_i.at[2 * b + h]) for h in order]

    for d in (1, 7, 2, 6, 3, 5, 4):
        send(U.at[mine], U.at[mine], s_u.at[mine], dev(dz=d))
    for d in (1, 3):
        send(U.at[mine], U.at[mine], s_u.at[mine], dev(dy=d))
    for dx, order in ((1, (0, 1)), (3, (1, 0))):
        for h, dst, sem in halves(bo, order):
            send(dst, dst, sem, dev(dx=dx))
    for h, dst, sem in halves(bo):
        send(dst, dst, sem, dev(dc=1))

    for d in (1, 7, 2, 6, 3, 5, 4):
        s = y * NZ + zz[d]
        arrived(U.at[s], s_u.at[s])
        for dy in (1, 3):
            send(U.at[s], U.at[s], s_u.at[s], dev(dy=dy))

    for dx, keep in ((3, 0), (1, 1)):
        b = c * NX + xx[dx]
        for h, ref, sem in halves(b, (keep, 1 - keep)):
            arrived(ref, sem)
            if h == keep:
                send(ref, ref, sem, dev(dx=4 - dx))
            send(ref, ref, sem, dev(dc=1))

    def place_ids(yi):
        UT[yi] = U[pl.ds(yi * NZ, NZ)].reshape(CH, E).T
        part = U[pl.ds(yi * NZ, NZ), OWN:ROW, 0:128].astype(F32)
        n = lax.broadcasted_iota(jnp.int32, (128, CH), 1)
        k = (n * 1366) >> 16
        pick = jnp.where(n - k * ROW == lax.broadcasted_iota(jnp.int32, (128, CH), 0), 1.0, 0.0)
        pick = pick.astype(BF16)
        n8 = lax.broadcasted_iota(jnp.int32, (NZ, CH), 1)
        k8 = (n8 * 1366) >> 16
        here = k8 == lax.broadcasted_iota(jnp.int32, (NZ, CH), 0)
        for j in range(2):
            spread = jnp.dot(part[:, j, :].astype(BF16), pick, preferred_element_type=F32)
            HL[yi, j] = jnp.sum(jnp.where(here, spread, 0.0), axis=0, keepdims=True)

    n1 = lax.broadcasted_iota(jnp.int32, (1, CH), 1)
    valid = n1 - ((n1 * 1366) >> 16) * ROW < OWN

    def target(yi, bx, bc):
        owner = (bx // 2) * 128 + z * 16 + lax.rem(bx, 2) * 8 + y * 2 + bc
        match = (HL[yi, 0] == owner.astype(F32)) & valid
        return jnp.where(match, HL[yi, 1], -1.0)

    rows = lax.broadcasted_iota(jnp.int32, (ITM, 128), 0).astype(F32)

    def logits(yi, b, lg):
        lg[...] = jnp.dot(I[b], UT[yi], preferred_element_type=F32)

    def exponents(yi, b, lg):
        at = target(yi, lax.rem(b, NX), b // NX)
        for j in range(CH // 128):
            cols = slice(128 * j, 128 * j + 128)
            part = lg[:, cols]
            top = jnp.max(part, axis=0, keepdims=True)
            ex = jnp.exp(part - top)
            EX[b, yi, :, cols] = ex
            MB[yi, b, :, cols] = top
            SB[yi, b, :, cols] = jnp.sum(ex, axis=0, keepdims=True)
            PB[yi, b, :, cols] = jnp.sum(jnp.where(rows == at[:, cols], part, 0.0), axis=0, keepdims=True)

    def first(yi, b):
        logits(yi, b, LGA)
        exponents(yi, b, LGA)

    def first_all(yi):
        logits(yi, 0, LGA)

        def two(i, _):
            logits(yi, 2 * i + 1, LGB)
            exponents(yi, 2 * i, LGA)
            logits(yi, lax.rem(2 * i + 2, NX * NC), LGA)
            exponents(yi, 2 * i + 1, LGB)
            return 0

        lax.fori_loop(0, NX * NC // 2, two, 0)

    def turn(b):
        IT[:, pl.ds(pl.multiple_of(b * ITM, ITM), ITM)] = I[b].T

    place_ids(yy[0])
    for dx in (0, 3, 1):
        b = c * NX + xx[dx]
        first(yy[0], b)
        turn(b)

    for dy, first_z in ((3, 0), (1, 1)):
        for d in range(NZ):
            s = yy[dy] * NZ + d
            arrived(U.at[s], s_u.at[s])
            if (d < NZ // 2) == (first_z == 0):
                send(U.at[s], U.at[s], s_u.at[s], dev(dy=4 - dy))

    b = c * NX + xx[2]
    for h, ref, sem in halves(b):
        arrived(ref, sem)
        send(ref, ref, sem, dev(dc=1))
    first(yy[0], b)
    turn(b)
    for dx in (0, 3, 1, 2):
        b = co * NX + xx[dx]
        for h, ref, sem in halves(b):
            arrived(ref, sem)
        first(yy[0], b)
        turn(b)

    for dy in (3, 1):
        place_ids(yy[dy])
        first_all(yy[dy])
    for d in range(NZ):
        s = yy[2] * NZ + d
        arrived(U.at[s], s_u.at[s])
    place_ids(yy[2])
    first_all(yy[2])

    NR = CH // 128
    for k in range(NY):
        m = jnp.max(MB[k], axis=0)
        s = jnp.sum(SB[k] * jnp.exp(MB[k] - m[None]), axis=0)
        line = m + jnp.log(s)
        p = jnp.sum(PB[k], axis=0)
        for j in range(NR):
            cols = slice(128 * j, 128 * j + 128)
            ST[NR * k + j : NR * k + j + 1] = line[:, cols]
            PT[k, j : j + 1] = p[:, cols]
        PT[k, NR:8] = jnp.zeros((8 - NR, 128), F32)
    ST[12:16] = jnp.zeros((4, 128), F32)

    def combine(parts):
        m = parts[0]
        for q in parts[1:]:
            m = jnp.maximum(m, q)
        s = jnp.zeros_like(m)
        for q in parts:
            s = s + jnp.exp(q - m)
        return m + jnp.log(s)

    for d in (2, 1, 3):
        send(ST, YST.at[y], s_ys.at[y], dev(dy=d))
    for d in (2, 1, 3):
        send(PT.at[yy[d]], YPT.at[y], s_yp.at[y], dev(dy=d))
    for d in (1, 3, 2):
        arrived(YST.at[yy[d]], s_ys.at[yy[d]])
    YST[y] = ST[...]
    ZST[z] = combine([YST[k] for k in range(NY)])
    for d in (4, 3, 5, 2, 6, 1, 7):
        send(ZST.at[z], ZST.at[z], s_zs.at[z], dev(dz=d))
    for d in (1, 3, 2):
        arrived(YPT.at[yy[d]], s_yp.at[yy[d]])
    ZPT[z] = PT[y] + YPT[yy[1]] + YPT[yy[2]] + YPT[yy[3]]
    for d in (4, 3, 5, 2, 6, 1, 7):
        send(ZPT.at[z], ZPT.at[z], s_zp.at[z], dev(dz=d))
    for d in (1, 7, 2, 6, 3, 5, 4):
        arrived(ZST.at[zz[d]], s_zs.at[zz[d]])
    lse = combine([ZST[k] for k in range(NZ)])
    for k in range(NY):
        for j in range(NR):
            r = NR * k + j
            SC[k, :, 128 * j : 128 * j + 128] = lse[r : r + 1]

    def span(yi):
        return pl.ds(pl.multiple_of(yi * CH, CH), CH)

    def second(yi, b):
        bx, bc = lax.rem(b, NX), b // NX
        at = target(yi, bx, bc)
        scale = jnp.where(valid, jnp.exp(MB[yi, b] - SC[yi]), 0.0)
        for j in range(CH // 128):
            cols = slice(128 * j, 128 * j + 128)
            w = EX[b, yi, :, cols] * scale[:, cols]
            w = w - jnp.where(rows == at[:, cols], 1.0, 0.0)
            W[bc, bx, :, pl.ds(pl.multiple_of(yi * CH + 128 * j, 128), 128)] = w.astype(BF16)

    def weights(yi):
        lax.fori_loop(0, NX * NC, lambda b, _: (second(yi, b), 0)[1], 0)

    def user_dot(d):
        w = W[:, :, :, span(yy[d])].reshape(NC * NX * ITM, CH)
        UG[d] = jnp.dot(IT[...], w, preferred_element_type=F32)

    def user_terms(d):
        weights(yy[d])
        user_dot(d)

    H = E // 2
    half = [pl.ds(0, H), pl.ds(H, H)]

    def send2(q, qto, m, mto, recv, i, where):
        send(q, qto, recv.at[i, 0], where)
        send(m, mto, recv.at[i, 1], where)

    def arrived2(q, m, recv, i):
        arrived(q, recv.at[i, 0])
        arrived(m, recv.at[i, 1])

    user_terms(2)
    for i in range(2):
        code(UG[2, H * i : H * i + H], QY2.at[i], MY2.at[i])
        send2(QY2.at[i], YQ2.at[i], MY2.at[i], YM2.at[i], s_y2, i, dev(dy=1 + 2 * i))

    def direct(d, i):
        h = 1 - i
        k = 2 * i + h
        code(UG[d, H * h : H * h + H], QY1.at[k], MY1.at[k])
        send2(QY1.at[k], YQ1.at[k], MY1.at[k], YM1.at[k], s_y1, k, dev(dy=d))

    def relayed(d, i):
        h = i
        k = 2 * i + h
        arrived2(YQ2.at[i], YM2.at[i], s_y2, i)
        code(UG[d, H * h : H * h + H] + decode(YQ2[i], YM2[i]), QY1.at[k], MY1.at[k])
        send2(QY1.at[k], YQ1.at[k], MY1.at[k], YM1.at[k], s_y1, k, dev(dy=d))

    user_terms(1)
    direct(1, 0)
    user_terms(3)
    direct(3, 1)
    weights(yy[0])
    relayed(1, 0)
    relayed(3, 1)

    everyone = NY * NZ * ROW

    def item_terms(bc, bx):
        w = W[bc, bx]
        G[bc * NX + bx] = jnp.dot(w, U[...].reshape(everyone, E), preferred_element_type=F32)

    for dx in (2, 1, 3, 0):
        item_terms(co, xx[dx])
        b = co * NX + xx[dx]
        code(G[b], QP.at[dx], MP.at[dx])
        send2(QP.at[dx], PQ.at[dx], MP.at[dx], PM.at[dx], s_pg, dx, dev(dc=1))
    user_dot(0)

    def own_terms(dx):
        b = c * NX + xx[dx]
        item_terms(c, xx[dx])
        arrived2(PQ.at[dx], PM.at[dx], s_pg, dx)
        G[b] += decode(PQ[dx], PM[dx])
        return b

    b2 = own_terms(2)
    for i in range(2):
        code(G[b2, H * i : H * i + H], QX2.at[i], MX2.at[i])
        send2(QX2.at[i], XQ2.at[i], MX2.at[i], XM2.at[i], s_x2, i, dev(dx=1 + 2 * i))

    def x_direct(dx, i):
        b = own_terms(dx)
        h = 1 - i
        k = 2 * i + h
        code(G[b, H * h : H * h + H], QX1.at[k], MX1.at[k])
        send2(QX1.at[k], XQ1.at[k], MX1.at[k], XM1.at[k], s_x1, k, dev(dx=dx))
        return b

    def x_relayed(b, dx, i):
        h = i
        k = 2 * i + h
        arrived2(XQ2.at[i], XM2.at[i], s_x2, i)
        code(G[b, H * h : H * h + H] + decode(XQ2[i], XM2[i]), QX1.at[k], MX1.at[k])
        send2(QX1.at[k], XQ1.at[k], MX1.at[k], XM1.at[k], s_x1, k, dev(dx=dx))

    b1 = x_direct(1, 0)
    b3 = x_direct(3, 1)
    total = []
    for h in range(2):
        v = UG[0, H * h : H * h + H]
        for i in range(2):
            k = 2 * i + h
            arrived2(YQ1.at[k], YM1.at[k], s_y1, k)
            v = v + decode(YQ1[k], YM1[k])
        UG[0, H * h : H * h + H] = v
    UZ[...] = UG[0].T.reshape(NZ, ROW, E)
    for d in (4, 3, 5, 2, 6, 1, 7):
        code(UZ[zz[d], 0:OWN], QZ.at[d], MZ.at[d])
        send2(QZ.at[d], ZQ.at[d], MZ.at[d], ZM.at[d], s_zr, d, dev(dz=d))

    x_relayed(b1, 1, 0)
    x_relayed(b3, 3, 1)
    b0 = own_terms(0)

    for d in (1, 7, 2, 6, 3, 5, 4):
        arrived(ZPT.at[zz[d]], s_zp.at[zz[d]])
    pos = ZPT[0]
    for k in range(1, NZ):
        pos = pos + ZPT[k]
    for j in range(NR):
        PB[0, 0, :, 128 * j : 128 * j + 128] = pos[j : j + 1]
    line = SC[y] - PB[0, 0]
    out = line[:, 0:ROW]
    for k in range(1, NZ):
        out = jnp.where(z == k, line[:, ROW * k : ROW * k + ROW], out)
    OL[:, 0:ROW] = out
    OL[:, ROW:128] = jnp.zeros((1, 128 - ROW), F32)
    loss_out[...] = OL[...]

    total = UZ[z, 0:OWN]
    for d in (1, 7, 2, 6, 3, 5, 4):
        arrived2(ZQ.at[d], ZM.at[d], s_zr, d)
        total = total + decode(ZQ[d], ZM[d])
    OU[...] = total
    ug_out[...] = OU[...]

    for h in range(2):
        v = G[b0, H * h : H * h + H]
        for i in range(2):
            k = 2 * i + h
            arrived2(XQ1.at[k], XM1.at[k], s_x1, k)
            v = v + decode(XQ1[k], XM1[k])
        OI[H * h : H * h + H] = v
        ig_out[H * h : H * h + H] = OI[H * h : H * h + H]

    for copy in sent:
        copy.wait_send()
    for copy in stored:
        copy.wait()


def finish(loss, ug, ig, loss_out, ug_out, ig_out, vl, sem):
    out = [pltpu.make_async_copy(a, b, sem.at[k]) for k, (a, b) in enumerate(((ig, ig_out), (ug, ug_out)))]
    for copy in out:
        copy.start()
    for copy in out:
        copy.wait()
    pltpu.sync_copy(loss, vl)
    loss_out[...] = vl[0, 0:OWN]


def local(users, items, pos_ids):
    V = pltpu.VMEM
    D = pltpu.SemaphoreType.DMA
    I16 = jnp.int16
    HE = E // 2
    scratch = [
        V((NY * NZ, ROW, E), BF16),
        V((NX * NC, ITM, E), BF16),
        V((1, OWN), jnp.int32),
        V((E, NX * NC * ITM), BF16),
        V((NY, E, CH), BF16),
        V((NY, 2, 1, CH), F32),
        V((ITM, CH), F32),
        V((ITM, CH), F32),
        V((NX * NC, NY, ITM, CH), F32),
        V((NY, NX * NC, 1, CH), F32),
        V((NY, NX * NC, 1, CH), F32),
        V((NY, NX * NC, 1, CH), F32),
        V((NC, NX, ITM, NY * CH), BF16),
        V((16, 128), F32),
        V((NY, 8, 128), F32),
        V((NY, 16, 128), F32),
        V((NY, 8, 128), F32),
        V((NZ, 16, 128), F32),
        V((NZ, 8, 128), F32),
        V((NY, 1, CH), F32),
        V((NY, E, CH), F32),
        V((NZ, ROW, E), F32),
        V((2, HE, CH), I16), V((2, 1, CH), F32),
        V((4, HE, CH), I16), V((4, 1, CH), F32),
        V((2, HE, CH), I16), V((2, 1, CH), F32),
        V((4, HE, CH), I16), V((4, 1, CH), F32),
        V((NZ, OWN, E), I16), V((NZ, 1, E), F32),
        V((NZ, OWN, E), I16), V((NZ, 1, E), F32),
        V((NX * NC, ITM, E), F32),
        V((NX, ITM, E), I16), V((NX, 1, E), F32),
        V((NX, ITM, E), I16), V((NX, 1, E), F32),
        V((2, HE, E), I16), V((2, 1, E), F32),
        V((4, HE, E), I16), V((4, 1, E), F32),
        V((2, HE, E), I16), V((2, 1, E), F32),
        V((4, HE, E), I16), V((4, 1, E), F32),
        V((1, 128), F32), V((OWN, E), F32), V((ITM, E), F32),
        D((3,)),
        D((4,)),
        D((1,)),
        D((NY * NZ,)),
        D((2 * NX * NC,)),
        D((NY,)), D((NY,)), D((NZ,)), D((NZ,)),
        D((2, 2)), D((4, 2)), D((NZ, 2)), D((NX, 2)), D((2, 2)), D((4, 2)),
    ]
    outs = (
        jax.ShapeDtypeStruct((1, 128), F32),
        jax.ShapeDtypeStruct((OWN, E), F32),
        jax.ShapeDtypeStruct((ITM, E), F32),
    )
    hbm = pl.BlockSpec(memory_space=pltpu.HBM)
    loss, ug, ig = pl.pallas_call(
        kernel,
        out_shape=tuple(pltpu.VMEM(o.shape, o.dtype) for o in outs),
        in_specs=[hbm] * 3,
        out_specs=tuple([pl.BlockSpec(memory_space=pltpu.VMEM)] * 3),
        scratch_shapes=scratch,
        compiler_params=pltpu.CompilerParams(
            collective_id=0, has_side_effects=True, vmem_limit_bytes=40 * 2**20
        ),
        name="infonce",
    )(*(pltpu.with_memory_space_constraint(a, pltpu.HBM) for a in (users, items, pos_ids.reshape(1, OWN))))
    return pl.pallas_call(
        finish,
        out_shape=(jax.ShapeDtypeStruct((OWN,), F32), *outs[1:]),
        in_specs=[pl.BlockSpec(memory_space=pl.ANY)] * 3,
        out_specs=(pl.BlockSpec(memory_space=pltpu.VMEM), hbm, hbm),
        scratch_shapes=[V((1, 128), F32), D((2,))],
        compiler_params=pltpu.CompilerParams(vmem_limit_bytes=2**20),
        name="finish",
    )(loss, ug, ig)


def solution(mesh):
    torus = Mesh(mesh.devices.reshape(2, NZ, 2, NY, NC), AXES)
    every = P(AXES)
    return jax.shard_map(
        local,
        mesh=torus,
        in_specs=(P(AXES, None), P(AXES, None), every),
        out_specs=(every, P(AXES, None), P(AXES, None)),
        check_vma=False,
    )
```

```python
import jax
import jax.numpy as jnp
from jax import lax
from jax.experimental import pallas as pl
from jax.experimental.pallas import tpu as pltpu
from jax.sharding import Mesh
from jax.sharding import PartitionSpec as P

AXES = ("xh", "z", "xl", "y", "c")
MESH = pl.DeviceIdType.MESH
F32 = jnp.float32
BF16 = jnp.bfloat16
NX, NY, NZ, NC = 4, 4, 8, 2
OWN = 40
ROW = 48
ITM = 256
E = 256
CH = NZ * ROW


TOP = 32704.0


def code(v, q, m):
    for j in range(v.shape[1] // 128):
        cols = slice(128 * j, 128 * j + 128)
        part = v[:, cols]
        most = jnp.maximum(jnp.max(jnp.abs(part), axis=0, keepdims=True), 1e-30)
        m[:, cols] = most
        q[:, cols] = jnp.round(part * (TOP / most)).astype(jnp.int16)


def decode(q, m):
    return q.astype(F32) * (m * (1.0 / TOP))


def kernel(users, items, ids, loss_out, ug_out, ig_out, U, I, ID, IT, UT, HL, LGA, LGB, EX, MB, SB, PB, W, ST, PT, YST, YPT, ZST, ZPT,
           SC, UG, UZ, QY2, MY2, QY1, MY1, YQ2, YM2, YQ1, YM1, QZ, MZ, ZQ, ZM, G, QP, MP, PQ, PM, QX2, MX2, QX1, MX1, XQ2, XM2,
           XQ1, XM1, OL, OU, OI, s_in, s_out, s_send, s_u, s_i, s_ys, s_yp, s_zs, s_zp, s_y2, s_y1, s_zr, s_pg, s_x2, s_x1):
    xh, z, xl, y, c = (lax.axis_index(a) for a in AXES)
    x = 2 * xh + xl

    def dev(dx=0, dy=0, dz=0, dc=0):
        nx = lax.rem(x + dx, NX)
        nc = lax.rem(c + dc, NC)
        return (nx // 2, lax.rem(z + dz, NZ), lax.rem(nx, 2), lax.rem(y + dy, NY), nc)

    sent = []

    def send(src, dst, recv, where):
        copy = pltpu.make_async_remote_copy(
            src_ref=src, dst_ref=dst, send_sem=s_send.at[0], recv_sem=recv,
            device_id=where, device_id_type=MESH,
        )
        copy.start()
        sent.append(copy)

    stored = []

    def store(src, dst, i):
        copy = pltpu.make_async_copy(src, dst, s_out.at[i])
        copy.start()
        stored.append(copy)

    def arrived(dst, recv):
        pltpu.make_async_remote_copy(
            src_ref=dst, dst_ref=dst, send_sem=s_send.at[0], recv_sem=recv,
            device_id=dev(dc=1), device_id_type=MESH,
        ).wait_recv()

    yy = [lax.rem(y + d, NY) for d in range(NY)]
    zz = [lax.rem(z + d, NZ) for d in range(NZ)]
    xx = [lax.rem(x + d, NX) for d in range(NX)]
    co = 1 - c

    mine = y * NZ + z
    bo = c * NX + x
    inputs = [
        pltpu.make_async_copy(users, U.at[mine, pl.ds(0, OWN)], s_in.at[0]),
        pltpu.make_async_copy(items, I.at[bo], s_in.at[1]),
        pltpu.make_async_copy(ids, ID, s_in.at[2]),
    ]
    for copy in inputs:
        copy.start()
    barrier = pltpu.get_barrier_semaphore()
    peers = [dict(dz=d) for d in range(1, NZ)] + [dict(dy=d) for d in range(1, NY)]
    peers += [dict(dx=1), dict(dx=3), dict(dc=1)]
    for p in peers:
        pl.semaphore_signal(barrier, inc=1, device_id=dev(**p), device_id_type=MESH)

    for copy in inputs:
        copy.wait()
    PB[0, 0] = jnp.zeros((1, CH), F32)
    PB[1, 0] = jnp.zeros((1, CH), F32)
    PB[0, 0, :, 0:OWN] = (ID[...] >> 8).astype(F32)
    PB[1, 0, :, 0:OWN] = (ID[...] & 255).astype(F32)
    r8 = lax.broadcasted_iota(jnp.int32, (ROW - OWN, E), 0)
    pad = jnp.where(r8 == 0, PB[0, 0, :, 0:E], jnp.where(r8 == 1, PB[1, 0, :, 0:E], 0.0))
    U[mine, OWN:ROW] = pad.astype(BF16)
    pl.semaphore_wait(barrier, len(peers))

    H = ITM // 2

    def halves(b, order=(0, 1)):
        return [(h, I.at[b, pl.ds(h * H, H)], s_i.at[2 * b + h]) for h in order]

    for d in (1, 7, 2, 6, 3, 5, 4):
        send(U.at[mine], U.at[mine], s_u.at[mine], dev(dz=d))
    for d in (1, 3):
        send(U.at[mine], U.at[mine], s_u.at[mine], dev(dy=d))
    for dx, order in ((1, (0, 1)), (3, (1, 0))):
        for h, dst, sem in halves(bo, order):
            send(dst, dst, sem, dev(dx=dx))
    for h, dst, sem in halves(bo):
        send(dst, dst, sem, dev(dc=1))

    def place_ids(yi):
        UT[yi] = U[pl.ds(yi * NZ, NZ)].reshape(CH, E).T
        part = U[pl.ds(yi * NZ, NZ), OWN:ROW, 0:128].astype(F32)
        n = lax.broadcasted_iota(jnp.int32, (128, CH), 1)
        k = (n * 1366) >> 16
        pick = jnp.where(n - k * ROW == lax.broadcasted_iota(jnp.int32, (128, CH), 0), 1.0, 0.0)
        pick = pick.astype(BF16)
        n8 = lax.broadcasted_iota(jnp.int32, (NZ, CH), 1)
        k8 = (n8 * 1366) >> 16
        here = k8 == lax.broadcasted_iota(jnp.int32, (NZ, CH), 0)
        for j in range(2):
            spread = jnp.dot(part[:, j, :].astype(BF16), pick, preferred_element_type=F32)
            HL[yi, j] = jnp.sum(jnp.where(here, spread, 0.0), axis=0, keepdims=True)

    n1 = lax.broadcasted_iota(jnp.int32, (1, CH), 1)
    valid = n1 - ((n1 * 1366) >> 16) * ROW < OWN

    def target(yi, bx, bc):
        owner = (bx // 2) * 128 + z * 16 + (bx % 2) * 8 + y * 2 + bc
        match = (HL[yi, 0] == owner.astype(F32)) & valid
        return jnp.where(match, HL[yi, 1], -1.0)

    rows = lax.broadcasted_iota(jnp.int32, (ITM, 128), 0).astype(F32)

    def logits(yi, b, n, lg):
        lg[0 : n * ITM] = jnp.dot(I[pl.ds(b, n)].reshape(n * ITM, E), UT[yi], preferred_element_type=F32)

    def exponents(yi, b, h, lg):
        at = target(yi, lax.rem(b, NX), b // NX)
        for j in range(CH // 128):
            cols = slice(128 * j, 128 * j + 128)
            part = lg[h * ITM : h * ITM + ITM, cols]
            top = jnp.max(part, axis=0, keepdims=True)
            ex = jnp.exp(part - top)
            EX[b, yi, :, cols] = ex
            MB[yi, b, :, cols] = top
            SB[yi, b, :, cols] = jnp.sum(ex, axis=0, keepdims=True)
            hit = jnp.zeros((8, 128), F32)
            for r in range(0, ITM, 8):
                hit = jnp.where(rows[r : r + 8] == at[:, cols], part[r : r + 8], hit)
            PB[yi, b, :, cols] = jnp.sum(hit, axis=0, keepdims=True)

    def first_some(yi, blocks):
        held = (LGA, LGB)
        logits(yi, blocks[0], 1, LGA)
        for k, b in enumerate(blocks):
            if k + 1 < len(blocks):
                logits(yi, blocks[k + 1], 1, held[(k + 1) % 2])
            exponents(yi, b, 0, held[k % 2])

    def first_all(yi):
        logits(yi, 0, 2, LGA)

        def four(i, _):
            logits(yi, 4 * i + 2, 2, LGB)
            exponents(yi, 4 * i, 0, LGA)
            exponents(yi, 4 * i + 1, 1, LGA)
            logits(yi, lax.rem(4 * i + 4, NX * NC), 2, LGA)
            exponents(yi, 4 * i + 2, 0, LGB)
            exponents(yi, 4 * i + 3, 1, LGB)
            return 0

        lax.fori_loop(0, NX * NC // 4, four, 0)

    def turn(b):
        IT[:, pl.ds(pl.multiple_of(b * ITM, ITM), ITM)] = I[b].T

    UP = (0, 7, 2, 5)

    def from_z(d):
        s = y * NZ + zz[d]
        arrived(U.at[s], s_u.at[s])
        for dy in (1, 3):
            send(U.at[s], U.at[s], s_u.at[s], dev(dy=dy))

    def from_y(d):
        for dy in (3, 1):
            s = yy[dy] * NZ + zz[d]
            arrived(U.at[s], s_u.at[s])
            if (d in UP) == (dy == 3):
                send(U.at[s], U.at[s], s_u.at[s], dev(dy=4 - dy))

    def from_x(step):
        for dx, keep in ((3, 0), (1, 1)):
            b = c * NX + xx[dx]
            h, ref, sem = halves(b, (keep, 1 - keep))[step]
            arrived(ref, sem)
            if step == 0:
                send(ref, ref, sem, dev(dx=4 - dx))
            send(ref, ref, sem, dev(dc=1))

    def from_x2():
        for h, ref, sem in halves(c * NX + xx[2]):
            arrived(ref, sem)
            send(ref, ref, sem, dev(dc=1))

    def from_partner(dx):
        b = co * NX + xx[dx]
        for h, ref, sem in halves(b):
            arrived(ref, sem)
        return b

    for d in (1, 7, 2, 6):
        from_z(d)
    from_y(0)
    from_x(0)
    for d in (3, 5, 4):
        from_z(d)
    from_x(1)
    place_ids(yy[0])
    first_some(yy[0], [c * NX + xx[dx] for dx in (0, 3, 1)])
    from_y(1)
    from_y(7)
    from_x2()
    from_y(2)
    from_y(6)
    first_some(yy[0], [from_partner(dx) for dx in (0, 3, 1)])
    for d in (3, 5, 4):
        from_y(d)
    first_some(yy[0], [c * NX + xx[2], from_partner(2)])

    for dy in (3, 1):
        place_ids(yy[dy])
        first_all(yy[dy])
    for d in range(NZ):
        s = yy[2] * NZ + d
        arrived(U.at[s], s_u.at[s])
    place_ids(yy[2])
    first_all(yy[2])

    NR = CH // 128
    for k in range(NY):
        m = jnp.max(MB[k], axis=0)
        s = jnp.sum(SB[k] * jnp.exp(MB[k] - m[None]), axis=0)
        line = m + jnp.log(s)
        p = jnp.sum(PB[k], axis=0)
        for j in range(NR):
            cols = slice(128 * j, 128 * j + 128)
            ST[NR * k + j : NR * k + j + 1] = line[:, cols]
            PT[k, j : j + 1] = p[:, cols]
        PT[k, NR:8] = jnp.zeros((8 - NR, 128), F32)
    ST[12:16] = jnp.zeros((4, 128), F32)

    def combine(parts):
        m = parts[0]
        for q in parts[1:]:
            m = jnp.maximum(m, q)
        s = jnp.zeros_like(m)
        for q in parts:
            s = s + jnp.exp(q - m)
        return m + jnp.log(s)

    for d in (2, 1, 3):
        send(ST, YST.at[y], s_ys.at[0], dev(dy=d))
    for d in (2, 1, 3):
        send(PT.at[yy[d]], YPT.at[y], s_yp.at[0], dev(dy=d))
    lax.fori_loop(0, NX * NC, lambda b, _: (turn(b), 0)[1], 0)
    arrived(YST.at[pl.ds(0, NY - 1)], s_ys.at[0])
    YST[y] = ST[...]
    ZST[z] = combine([YST[k] for k in range(NY)])
    for d in (4, 3, 5, 2, 6, 1, 7):
        send(ZST.at[z], ZST.at[z], s_zs.at[0], dev(dz=d))
    arrived(YPT.at[pl.ds(0, NY - 1)], s_yp.at[0])
    ZPT[z] = PT[y] + YPT[yy[1]] + YPT[yy[2]] + YPT[yy[3]]
    for d in (4, 3, 5, 2, 6, 1, 7):
        send(ZPT.at[z], ZPT.at[z], s_zp.at[0], dev(dz=d))
    arrived(ZST.at[pl.ds(0, NZ - 1)], s_zs.at[0])
    lse = combine([ZST[k] for k in range(NZ)])
    for k in range(NY):
        for j in range(NR):
            r = NR * k + j
            SC[k, :, 128 * j : 128 * j + 128] = lse[r : r + 1]

    def span(yi):
        return pl.ds(pl.multiple_of(yi * CH, CH), CH)

    def second(yi, b):
        bx, bc = b % NX, b // NX
        at = target(yi, bx, bc)
        scale = jnp.where(valid, jnp.exp(MB[yi, b] - SC[yi]), 0.0)
        for j in range(CH // 128):
            cols = slice(128 * j, 128 * j + 128)
            w = EX[b, yi, :, cols] * scale[:, cols]
            w = w - jnp.where(rows == at[:, cols], 1.0, 0.0)
            W[bc, bx, :, pl.ds(pl.multiple_of(yi * CH + 128 * j, 128), 128)] = w.astype(BF16)

    def weights(yi):
        for b in range(NX * NC):
            second(yi, b)

    def user_dot(d):
        w = W[:, :, :, span(yy[d])].reshape(NC * NX * ITM, CH)
        UG[d] = jnp.dot(IT[...], w, preferred_element_type=F32)

    def user_terms(d):
        weights(yy[d])
        user_dot(d)

    H = E // 2
    half = [pl.ds(0, H), pl.ds(H, H)]

    def send2(q, qto, m, mto, recv, i, where):
        send(q, qto, recv.at[i, 0], where)
        send(m, mto, recv.at[i, 1], where)

    def arrived2(q, m, recv, i):
        arrived(q, recv.at[i, 0])
        arrived(m, recv.at[i, 1])

    user_terms(2)
    for i in range(2):
        code(UG[2, H * i : H * i + H], QY2.at[i], MY2.at[i])
        send2(QY2.at[i], YQ2.at[i], MY2.at[i], YM2.at[i], s_y2, i, dev(dy=1 + 2 * i))

    def direct(d, i):
        h = 1 - i
        k = 2 * i + h
        code(UG[d, H * h : H * h + H], QY1.at[k], MY1.at[k])
        send2(QY1.at[k], YQ1.at[k], MY1.at[k], YM1.at[k], s_y1, 0, dev(dy=d))

    def relayed(d, i):
        h = i
        k = 2 * i + h
        arrived2(YQ2.at[i], YM2.at[i], s_y2, i)
        code(UG[d, H * h : H * h + H] + decode(YQ2[i], YM2[i]), QY1.at[k], MY1.at[k])
        send2(QY1.at[k], YQ1.at[k], MY1.at[k], YM1.at[k], s_y1, 0, dev(dy=d))

    user_terms(1)
    direct(1, 0)
    user_terms(3)
    direct(3, 1)
    everyone = NY * NZ * ROW

    def item_terms(bc, bx):
        w = W[bc, bx]
        G[bc * NX + bx] = jnp.dot(w, U[...].reshape(everyone, E), preferred_element_type=F32)

    def partner_terms(dx):
        item_terms(co, xx[dx])
        b = co * NX + xx[dx]
        code(G[b], QP.at[dx], MP.at[dx])
        send2(QP.at[dx], PQ.at[dx], MP.at[dx], PM.at[dx], s_pg, dx, dev(dc=1))

    def add_partner(dx):
        b = c * NX + xx[dx]
        arrived2(PQ.at[dx], PM.at[dx], s_pg, dx)
        G[b] += decode(PQ[dx], PM[dx])
        return b

    def own_terms(dx):
        item_terms(c, xx[dx])
        return add_partner(dx)

    weights(yy[0])
    partner_terms(2)
    relayed(1, 0)
    relayed(3, 1)
    item_terms(c, xx[2])
    partner_terms(1)
    b2 = add_partner(2)
    for i in range(2):
        code(G[b2, H * i : H * i + H], QX2.at[i], MX2.at[i])
        send2(QX2.at[i], XQ2.at[i], MX2.at[i], XM2.at[i], s_x2, i, dev(dx=1 + 2 * i))
    partner_terms(3)

    def x_direct(dx, i):
        b = own_terms(dx)
        h = 1 - i
        k = 2 * i + h
        code(G[b, H * h : H * h + H], QX1.at[k], MX1.at[k])
        send2(QX1.at[k], XQ1.at[k], MX1.at[k], XM1.at[k], s_x1, 0, dev(dx=dx))
        return b

    def x_relayed(b, dx, i):
        h = i
        k = 2 * i + h
        arrived2(XQ2.at[i], XM2.at[i], s_x2, i)
        code(G[b, H * h : H * h + H] + decode(XQ2[i], XM2[i]), QX1.at[k], MX1.at[k])
        send2(QX1.at[k], XQ1.at[k], MX1.at[k], XM1.at[k], s_x1, 0, dev(dx=dx))

    user_dot(0)
    b1 = x_direct(1, 0)
    total = []
    arrived2(YQ1, YM1, s_y1, 0)
    for h in range(2):
        v = UG[0, H * h : H * h + H]
        for i in range(2):
            k = 2 * i + h
            v = v + decode(YQ1[k], YM1[k])
        UG[0, H * h : H * h + H] = v
    UZ[...] = UG[0].T.reshape(NZ, ROW, E)
    for d in (4, 3, 5, 2, 6, 1, 7):
        code(UZ[zz[d], 0:OWN], QZ.at[d], MZ.at[d])
        send2(QZ.at[d], ZQ.at[d], MZ.at[d], ZM.at[d], s_zr, 0, dev(dz=d))

    partner_terms(0)
    b3 = x_direct(3, 1)
    x_relayed(b1, 1, 0)
    x_relayed(b3, 3, 1)
    b0 = own_terms(0)

    arrived(ZPT.at[pl.ds(0, NZ - 1)], s_zp.at[0])
    pos = ZPT[0]
    for k in range(1, NZ):
        pos = pos + ZPT[k]
    for j in range(NR):
        PB[0, 0, :, 128 * j : 128 * j + 128] = pos[j : j + 1]
    line = SC[y] - PB[0, 0]
    out = line[:, 0:ROW]
    for k in range(1, NZ):
        out = jnp.where(z == k, line[:, ROW * k : ROW * k + ROW], out)
    OL[:, 0:ROW] = out
    OL[:, ROW:128] = jnp.zeros((1, 128 - ROW), F32)
    loss_out[...] = OL[...]

    total = UZ[z, 0:OWN]
    arrived2(ZQ.at[pl.ds(1, NZ - 1)], ZM.at[pl.ds(1, NZ - 1)], s_zr, 0)
    for d in range(1, NZ):
        total = total + decode(ZQ[d], ZM[d])
    OU[...] = total
    ug_out[...] = OU[...]

    arrived2(XQ1, XM1, s_x1, 0)
    for h in range(2):
        v = G[b0, H * h : H * h + H]
        for i in range(2):
            k = 2 * i + h
            v = v + decode(XQ1[k], XM1[k])
        OI[H * h : H * h + H] = v
        ig_out[H * h : H * h + H] = OI[H * h : H * h + H]

    for copy in sent:
        copy.wait_send()
    for copy in stored:
        copy.wait()


def finish(loss, ug, ig, loss_out, ug_out, ig_out, vl, sem):
    out = [pltpu.make_async_copy(a, b, sem.at[k]) for k, (a, b) in enumerate(((ig, ig_out), (ug, ug_out)))]
    for copy in out:
        copy.start()
    for copy in out:
        copy.wait()
    pltpu.sync_copy(loss, vl)
    loss_out[...] = vl[0, 0:OWN]


def local(users, items, pos_ids):
    V = pltpu.VMEM
    D = pltpu.SemaphoreType.DMA
    I16 = jnp.int16
    HE = E // 2
    scratch = [
        V((NY * NZ, ROW, E), BF16),
        V((NX * NC, ITM, E), BF16),
        V((1, OWN), jnp.int32),
        V((E, NX * NC * ITM), BF16),
        V((NY, E, CH), BF16),
        V((NY, 2, 1, CH), F32),
        V((2 * ITM, CH), F32),
        V((2 * ITM, CH), F32),
        V((NX * NC, NY, ITM, CH), F32),
        V((NY, NX * NC, 1, CH), F32),
        V((NY, NX * NC, 1, CH), F32),
        V((NY, NX * NC, 1, CH), F32),
        V((NC, NX, ITM, NY * CH), BF16),
        V((16, 128), F32),
        V((NY, 8, 128), F32),
        V((NY, 16, 128), F32),
        V((NY, 8, 128), F32),
        V((NZ, 16, 128), F32),
        V((NZ, 8, 128), F32),
        V((NY, 1, CH), F32),
        V((NY, E, CH), F32),
        V((NZ, ROW, E), F32),
        V((2, HE, CH), I16), V((2, 1, CH), F32),
        V((4, HE, CH), I16), V((4, 1, CH), F32),
        V((2, HE, CH), I16), V((2, 1, CH), F32),
        V((4, HE, CH), I16), V((4, 1, CH), F32),
        V((NZ, OWN, E), I16), V((NZ, 1, E), F32),
        V((NZ, OWN, E), I16), V((NZ, 1, E), F32),
        V((NX * NC, ITM, E), F32),
        V((NX, ITM, E), I16), V((NX, 1, E), F32),
        V((NX, ITM, E), I16), V((NX, 1, E), F32),
        V((2, HE, E), I16), V((2, 1, E), F32),
        V((4, HE, E), I16), V((4, 1, E), F32),
        V((2, HE, E), I16), V((2, 1, E), F32),
        V((4, HE, E), I16), V((4, 1, E), F32),
        V((1, 128), F32), V((OWN, E), F32), V((ITM, E), F32),
        D((3,)),
        D((4,)),
        D((1,)),
        D((NY * NZ,)),
        D((2 * NX * NC,)),
        D((1,)), D((1,)), D((1,)), D((1,)),
        D((2, 2)), D((1, 2)), D((1, 2)), D((NX, 2)), D((2, 2)), D((1, 2)),
    ]
    outs = (
        jax.ShapeDtypeStruct((1, 128), F32),
        jax.ShapeDtypeStruct((OWN, E), F32),
        jax.ShapeDtypeStruct((ITM, E), F32),
    )
    hbm = pl.BlockSpec(memory_space=pltpu.HBM)
    loss, ug, ig = pl.pallas_call(
        kernel,
        out_shape=tuple(pltpu.VMEM(o.shape, o.dtype) for o in outs),
        in_specs=[hbm] * 3,
        out_specs=tuple([pl.BlockSpec(memory_space=pltpu.VMEM)] * 3),
        scratch_shapes=scratch,
        compiler_params=pltpu.CompilerParams(
            collective_id=0, has_side_effects=True, vmem_limit_bytes=40 * 2**20
        ),
        name="infonce",
    )(*(pltpu.with_memory_space_constraint(a, pltpu.HBM) for a in (users, items, pos_ids.reshape(1, OWN))))
    return pl.pallas_call(
        finish,
        out_shape=(jax.ShapeDtypeStruct((OWN,), F32), *outs[1:]),
        in_specs=[pl.BlockSpec(memory_space=pl.ANY)] * 3,
        out_specs=(pl.BlockSpec(memory_space=pltpu.VMEM), hbm, hbm),
        scratch_shapes=[V((1, 128), F32), D((2,))],
        compiler_params=pltpu.CompilerParams(vmem_limit_bytes=2**20),
        name="finish",
    )(loss, ug, ig)


def solution(mesh):
    torus = Mesh(mesh.devices.reshape(2, NZ, 2, NY, NC), AXES)
    every = P(AXES)
    return jax.shard_map(
        local,
        mesh=torus,
        in_specs=(P(AXES, None), P(AXES, None), every),
        out_specs=(every, P(AXES, None), P(AXES, None)),
        check_vma=False,
    )
```

```python
import jax
import jax.numpy as jnp
from jax import lax
from jax.experimental import pallas as pl
from jax.experimental.pallas import tpu as pltpu
from jax.sharding import Mesh
from jax.sharding import PartitionSpec as P

AXES = ("xh", "z", "xl", "y", "c")
MESH = pl.DeviceIdType.MESH
F32 = jnp.float32
BF16 = jnp.bfloat16
NX, NY, NZ, NC = 4, 4, 8, 2
OWN = 40
ROW = 48
ITM = 256
E = 256
CH = NZ * ROW


TOP = 32704.0


def code(v, q, m):
    for j in range(v.shape[1] // 128):
        cols = slice(128 * j, 128 * j + 128)
        part = v[:, cols]
        most = jnp.maximum(jnp.max(jnp.abs(part), axis=0, keepdims=True), 1e-30)
        m[:, cols] = most
        q[:, cols] = jnp.round(part * (TOP / most)).astype(jnp.int16)


def decode(q, m):
    return q.astype(F32) * (m * (1.0 / TOP))


def kernel(users, items, ids, loss_out, ug_out, ig_out, U, I, ID, IDS, IT, UT, HL, LGA, LGB, EX, MB, SB, PB, W, ST, PT, YST, YPT, ZST, ZPT,
           SC, UG, QY2, MY2, QY1, MY1, YQ2, YM2, YQ1, YM1, QZ, MZ, ZQ, ZM, G, QP, MP, PQ, PM, QX2, MX2, QX1, MX1, XQ2, XM2,
           XQ1, XM1, OL, OU, OI, s_in, s_out, s_send, s_iz, s_iy, s_u, s_i, s_ys, s_yp, s_zs, s_zp, s_y2, s_y1, s_zr, s_pg, s_x2, s_x1):
    xh, z, xl, y, c = (lax.axis_index(a) for a in AXES)
    x = 2 * xh + xl

    def dev(dx=0, dy=0, dz=0, dc=0):
        nx = lax.rem(x + dx, NX)
        nc = lax.rem(c + dc, NC)
        return (nx // 2, lax.rem(z + dz, NZ), lax.rem(nx, 2), lax.rem(y + dy, NY), nc)

    sent = []

    def send(src, dst, recv, where):
        copy = pltpu.make_async_remote_copy(
            src_ref=src, dst_ref=dst, send_sem=s_send.at[0], recv_sem=recv,
            device_id=where, device_id_type=MESH,
        )
        copy.start()
        sent.append(copy)

    stored = []

    def store(src, dst, i):
        copy = pltpu.make_async_copy(src, dst, s_out.at[i])
        copy.start()
        stored.append(copy)

    def arrived(dst, recv):
        pltpu.make_async_remote_copy(
            src_ref=dst, dst_ref=dst, send_sem=s_send.at[0], recv_sem=recv,
            device_id=dev(dc=1), device_id_type=MESH,
        ).wait_recv()

    yy = [lax.rem(y + d, NY) for d in range(NY)]
    zz = [lax.rem(z + d, NZ) for d in range(NZ)]
    xx = [lax.rem(x + d, NX) for d in range(NX)]
    co = 1 - c

    mine = y * NZ + z
    bo = c * NX + x
    inputs = [
        pltpu.make_async_copy(users, U.at[mine, pl.ds(0, OWN)], s_in.at[0]),
        pltpu.make_async_copy(items, I.at[bo], s_in.at[1]),
        pltpu.make_async_copy(ids, ID, s_in.at[2]),
    ]
    for copy in inputs:
        copy.start()
    U[:, OWN:ROW] = jnp.zeros((NY * NZ, ROW - OWN, E), BF16)
    barrier = pltpu.get_barrier_semaphore()
    peers = [dict(dz=d) for d in range(1, NZ)] + [dict(dy=d) for d in range(1, NY)]
    peers += [dict(dx=1), dict(dx=3), dict(dc=1)]
    for p in peers:
        pl.semaphore_signal(barrier, inc=1, device_id=dev(**p), device_id_type=MESH)

    for copy in inputs:
        copy.wait()
    IDS[mine] = jnp.zeros((1, 128), jnp.int32)
    IDS[mine, :, 0:OWN] = ID[...]
    pl.semaphore_wait(barrier, len(peers))

    H = ITM // 2

    def halves(b, order=(0, 1)):
        return [(h, I.at[b, pl.ds(h * H, H)], s_i.at[2 * b + h]) for h in order]

    def send_users(s, where):
        block = U.at[s, pl.ds(0, OWN)]
        send(block, block, s_u.at[s], where)

    def users_arrived(s):
        arrived(U.at[s, pl.ds(0, OWN)], s_u.at[s])

    for d in (1, 7, 2, 6, 3, 5, 4):
        send_users(mine, dev(dz=d))
    for d in (1, 3):
        send_users(mine, dev(dy=d))
    for d in range(1, NZ):
        send(IDS.at[mine], IDS.at[mine], s_iz.at[0], dev(dz=d))
    for dx, order in ((1, (0, 1)), (3, (1, 0))):
        for h, dst, sem in halves(bo, order):
            send(dst, dst, sem, dev(dx=dx))
    for h, dst, sem in halves(bo):
        send(dst, dst, sem, dev(dc=1))

    def place_ids(yi):
        UT[yi] = U[pl.ds(yi * NZ, NZ)].reshape(CH, E).T
        part = IDS[pl.ds(yi * NZ, NZ)].reshape(NZ, 128)
        parts = (part >> 8, part & 255)
        n = lax.broadcasted_iota(jnp.int32, (128, CH), 1)
        k = (n * 1366) >> 16
        pick = jnp.where(n - k * ROW == lax.broadcasted_iota(jnp.int32, (128, CH), 0), 1.0, 0.0)
        pick = pick.astype(BF16)
        n8 = lax.broadcasted_iota(jnp.int32, (NZ, CH), 1)
        k8 = (n8 * 1366) >> 16
        here = k8 == lax.broadcasted_iota(jnp.int32, (NZ, CH), 0)
        for j in range(2):
            spread = jnp.dot(parts[j].astype(F32).astype(BF16), pick, preferred_element_type=F32)
            HL[yi, j] = jnp.sum(jnp.where(here, spread, 0.0), axis=0, keepdims=True)

    n1 = lax.broadcasted_iota(jnp.int32, (1, CH), 1)
    valid = n1 - ((n1 * 1366) >> 16) * ROW < OWN

    def target(yi, bx, bc):
        owner = (bx // 2) * 128 + z * 16 + (bx % 2) * 8 + y * 2 + bc
        match = (HL[yi, 0] == owner.astype(F32)) & valid
        return jnp.where(match, HL[yi, 1], -1.0)

    rows = lax.broadcasted_iota(jnp.int32, (ITM, 128), 0).astype(F32)

    def logits(yi, b, n, lg):
        lg[0 : n * ITM] = jnp.dot(I[pl.ds(b, n)].reshape(n * ITM, E), UT[yi], preferred_element_type=F32)

    def exponents(yi, b, h, lg):
        at = target(yi, lax.rem(b, NX), b // NX)
        for j in range(CH // 128):
            cols = slice(128 * j, 128 * j + 128)
            part = lg[h * ITM : h * ITM + ITM, cols]
            top = jnp.max(part, axis=0, keepdims=True)
            ex = jnp.exp(part - top)
            EX[b, yi, :, cols] = ex
            MB[yi, b, :, cols] = top
            SB[yi, b, :, cols] = jnp.sum(ex, axis=0, keepdims=True)
            hit = jnp.zeros((8, 128), F32)
            for r in range(0, ITM, 8):
                hit = jnp.where(rows[r : r + 8] == at[:, cols], part[r : r + 8], hit)
            PB[yi, b, :, cols] = jnp.sum(hit, axis=0, keepdims=True)

    def first_some(yi, blocks):
        held = (LGA, LGB)
        logits(yi, blocks[0], 1, LGA)
        for k, b in enumerate(blocks):
            if k + 1 < len(blocks):
                logits(yi, blocks[k + 1], 1, held[(k + 1) % 2])
            exponents(yi, b, 0, held[k % 2])

    def first_all(yi):
        logits(yi, 0, 2, LGA)

        def four(i, _):
            logits(yi, 4 * i + 2, 2, LGB)
            exponents(yi, 4 * i, 0, LGA)
            exponents(yi, 4 * i + 1, 1, LGA)
            logits(yi, lax.rem(4 * i + 4, NX * NC), 2, LGA)
            exponents(yi, 4 * i + 2, 0, LGB)
            exponents(yi, 4 * i + 3, 1, LGB)
            return 0

        lax.fori_loop(0, NX * NC // 4, four, 0)

    def turn(b):
        IT[:, pl.ds(pl.multiple_of(b * ITM, ITM), ITM)] = I[b].T

    UP = (0, 7, 2, 5)

    def from_z(d):
        s = y * NZ + zz[d]
        users_arrived(s)
        for dy in (1, 3):
            send_users(s, dev(dy=dy))

    def from_y(d):
        for dy in (3, 1):
            s = yy[dy] * NZ + zz[d]
            users_arrived(s)
            if (d in UP) == (dy == 3):
                send_users(s, dev(dy=4 - dy))

    def from_x(step):
        for dx, keep in ((3, 0), (1, 1)):
            b = c * NX + xx[dx]
            h, ref, sem = halves(b, (keep, 1 - keep))[step]
            arrived(ref, sem)
            if step == 0:
                send(ref, ref, sem, dev(dx=4 - dx))
            send(ref, ref, sem, dev(dc=1))

    def from_x2():
        for h, ref, sem in halves(c * NX + xx[2]):
            arrived(ref, sem)
            send(ref, ref, sem, dev(dc=1))

    def from_partner(dx):
        b = co * NX + xx[dx]
        for h, ref, sem in halves(b):
            arrived(ref, sem)
        return b

    for d in (1, 7, 2):
        from_z(d)
    from_x(0)
    from_z(6)
    from_y(0)
    from_z(3)
    from_x(1)
    from_z(5)
    from_z(4)
    arrived(IDS.at[pl.ds(0, NZ - 1)], s_iz.at[0])
    these = IDS.at[pl.ds(y * NZ, NZ)]
    for dy in (1, 3, 2):
        send(these, these, s_iy.at[0], dev(dy=dy))
    place_ids(yy[0])
    first_some(yy[0], [c * NX + xx[dx] for dx in (0, 3, 1)])
    first_some(yy[0], [from_partner(dx) for dx in (0, 3, 1)])
    for d in (1, 7):
        from_y(d)
    from_x2()
    for d in (2, 6, 3, 5, 4):
        from_y(d)
    first_some(yy[0], [c * NX + xx[2], from_partner(2)])

    arrived(IDS.at[pl.ds(0, (NY - 1) * NZ)], s_iy.at[0])
    for dy in (3, 1):
        place_ids(yy[dy])
        first_all(yy[dy])
    for d in range(NZ):
        users_arrived(yy[2] * NZ + d)
    place_ids(yy[2])
    first_all(yy[2])

    NR = CH // 128
    for k in range(NY):
        m = jnp.max(MB[k], axis=0)
        s = jnp.sum(SB[k] * jnp.exp(MB[k] - m[None]), axis=0)
        line = m + jnp.log(s)
        p = jnp.sum(PB[k], axis=0)
        for j in range(NR):
            cols = slice(128 * j, 128 * j + 128)
            ST[NR * k + j : NR * k + j + 1] = line[:, cols]
            PT[k, j : j + 1] = p[:, cols]
        PT[k, NR:8] = jnp.zeros((8 - NR, 128), F32)
    ST[12:16] = jnp.zeros((4, 128), F32)

    def combine(parts):
        m = parts[0]
        for q in parts[1:]:
            m = jnp.maximum(m, q)
        s = jnp.zeros_like(m)
        for q in parts:
            s = s + jnp.exp(q - m)
        return m + jnp.log(s)

    for d in (2, 1, 3):
        send(ST, YST.at[y], s_ys.at[0], dev(dy=d))
    for d in (2, 1, 3):
        send(PT.at[yy[d]], YPT.at[y], s_yp.at[0], dev(dy=d))
    lax.fori_loop(0, NX * NC, lambda b, _: (turn(b), 0)[1], 0)
    arrived(YST.at[pl.ds(0, NY - 1)], s_ys.at[0])
    YST[y] = ST[...]
    ZST[z] = combine([YST[k] for k in range(NY)])
    for d in (4, 3, 5, 2, 6, 1, 7):
        send(ZST.at[z], ZST.at[z], s_zs.at[0], dev(dz=d))
    arrived(YPT.at[pl.ds(0, NY - 1)], s_yp.at[0])
    ZPT[z] = PT[y] + YPT[yy[1]] + YPT[yy[2]] + YPT[yy[3]]
    for d in (4, 3, 5, 2, 6, 1, 7):
        send(ZPT.at[z], ZPT.at[z], s_zp.at[0], dev(dz=d))
    arrived(ZST.at[pl.ds(0, NZ - 1)], s_zs.at[0])
    lse = combine([ZST[k] for k in range(NZ)])
    for k in range(NY):
        for j in range(NR):
            r = NR * k + j
            SC[k, :, 128 * j : 128 * j + 128] = lse[r : r + 1]

    def span(yi):
        return pl.ds(pl.multiple_of(yi * CH, CH), CH)

    def second(yi, b):
        bx, bc = b % NX, b // NX
        at = target(yi, bx, bc)
        scale = jnp.where(valid, jnp.exp(MB[yi, b] - SC[yi]), 0.0)
        for j in range(CH // 128):
            cols = slice(128 * j, 128 * j + 128)
            w = EX[b, yi, :, cols] * scale[:, cols]
            w = w - jnp.where(rows == at[:, cols], 1.0, 0.0)
            W[bc, bx, :, pl.ds(pl.multiple_of(yi * CH + 128 * j, 128), 128)] = w.astype(BF16)

    def weights(yi):
        for b in range(NX * NC):
            second(yi, b)

    def user_dot(d):
        w = W[:, :, :, span(yy[d])].reshape(NC * NX * ITM, CH)
        UG[d] = jnp.dot(IT[...], w, preferred_element_type=F32).T.reshape(NZ, ROW, E)

    def user_terms(d):
        weights(yy[d])
        user_dot(d)

    H = ITM // 2
    HZ = NZ // 2

    def part(d, h):
        return UG[d, HZ * h : HZ * h + HZ, 0:OWN].reshape(HZ * OWN, E)

    def send2(q, qto, m, mto, recv, i, where):
        send(q, qto, recv.at[i, 0], where)
        send(m, mto, recv.at[i, 1], where)

    def arrived2(q, m, recv, i):
        arrived(q, recv.at[i, 0])
        arrived(m, recv.at[i, 1])

    user_terms(2)
    for i in range(2):
        code(part(2, i), QY2.at[i], MY2.at[i])
        send2(QY2.at[i], YQ2.at[i], MY2.at[i], YM2.at[i], s_y2, i, dev(dy=1 + 2 * i))

    def direct(d, i):
        h = 1 - i
        k = 2 * i + h
        code(part(d, h), QY1.at[k], MY1.at[k])
        send2(QY1.at[k], YQ1.at[k], MY1.at[k], YM1.at[k], s_y1, 0, dev(dy=d))

    def relayed(d, i):
        h = i
        k = 2 * i + h
        arrived2(YQ2.at[i], YM2.at[i], s_y2, i)
        code(part(d, h) + decode(YQ2[i], YM2[i]), QY1.at[k], MY1.at[k])
        send2(QY1.at[k], YQ1.at[k], MY1.at[k], YM1.at[k], s_y1, 0, dev(dy=d))

    user_terms(1)
    direct(1, 0)
    user_terms(3)
    direct(3, 1)
    everyone = NY * NZ * ROW

    def item_terms(bc, bx):
        w = W[bc, bx]
        G[bc * NX + bx] = jnp.dot(w, U[...].reshape(everyone, E), preferred_element_type=F32)

    def partner_terms(dx):
        item_terms(co, xx[dx])
        b = co * NX + xx[dx]
        code(G[b], QP.at[dx], MP.at[dx])
        send2(QP.at[dx], PQ.at[dx], MP.at[dx], PM.at[dx], s_pg, dx, dev(dc=1))

    def add_partner(dx):
        b = c * NX + xx[dx]
        arrived2(PQ.at[dx], PM.at[dx], s_pg, dx)
        G[b] += decode(PQ[dx], PM[dx])
        return b

    def own_terms(dx):
        item_terms(c, xx[dx])
        return add_partner(dx)

    weights(yy[0])
    partner_terms(2)
    relayed(1, 0)
    relayed(3, 1)
    item_terms(c, xx[2])
    partner_terms(1)
    b2 = add_partner(2)
    for i in range(2):
        code(G[b2, H * i : H * i + H], QX2.at[i], MX2.at[i])
        send2(QX2.at[i], XQ2.at[i], MX2.at[i], XM2.at[i], s_x2, i, dev(dx=1 + 2 * i))
    partner_terms(3)

    def x_direct(dx, i):
        b = own_terms(dx)
        h = 1 - i
        k = 2 * i + h
        code(G[b, H * h : H * h + H], QX1.at[k], MX1.at[k])
        send2(QX1.at[k], XQ1.at[k], MX1.at[k], XM1.at[k], s_x1, 0, dev(dx=dx))
        return b

    def x_relayed(b, dx, i):
        h = i
        k = 2 * i + h
        arrived2(XQ2.at[i], XM2.at[i], s_x2, i)
        code(G[b, H * h : H * h + H] + decode(XQ2[i], XM2[i]), QX1.at[k], MX1.at[k])
        send2(QX1.at[k], XQ1.at[k], MX1.at[k], XM1.at[k], s_x1, 0, dev(dx=dx))

    user_dot(0)
    b1 = x_direct(1, 0)
    arrived2(YQ1, YM1, s_y1, 0)
    for h in range(2):
        v = part(0, h)
        for i in range(2):
            k = 2 * i + h
            v = v + decode(YQ1[k], YM1[k])
        UG[0, HZ * h : HZ * h + HZ, 0:OWN] = v.reshape(HZ, OWN, E)
    for d in (4, 3, 5, 2, 6, 1, 7):
        code(UG[0, zz[d], 0:OWN], QZ.at[d], MZ.at[d])
        send2(QZ.at[d], ZQ.at[d], MZ.at[d], ZM.at[d], s_zr, 0, dev(dz=d))

    partner_terms(0)
    b3 = x_direct(3, 1)
    x_relayed(b1, 1, 0)
    x_relayed(b3, 3, 1)
    b0 = own_terms(0)

    arrived(ZPT.at[pl.ds(0, NZ - 1)], s_zp.at[0])
    pos = ZPT[0]
    for k in range(1, NZ):
        pos = pos + ZPT[k]
    for j in range(NR):
        PB[0, 0, :, 128 * j : 128 * j + 128] = pos[j : j + 1]
    line = SC[y] - PB[0, 0]
    out = line[:, 0:ROW]
    for k in range(1, NZ):
        out = jnp.where(z == k, line[:, ROW * k : ROW * k + ROW], out)
    OL[:, 0:ROW] = out
    OL[:, ROW:128] = jnp.zeros((1, 128 - ROW), F32)
    loss_out[...] = OL[...]

    total = UG[0, z, 0:OWN]
    arrived2(ZQ.at[pl.ds(1, NZ - 1)], ZM.at[pl.ds(1, NZ - 1)], s_zr, 0)
    for d in range(1, NZ):
        total = total + decode(ZQ[d], ZM[d])
    OU[...] = total
    ug_out[...] = OU[...]

    arrived2(XQ1, XM1, s_x1, 0)
    for h in range(2):
        v = G[b0, H * h : H * h + H]
        for i in range(2):
            k = 2 * i + h
            v = v + decode(XQ1[k], XM1[k])
        OI[H * h : H * h + H] = v
        ig_out[H * h : H * h + H] = OI[H * h : H * h + H]

    for copy in sent:
        copy.wait_send()
    for copy in stored:
        copy.wait()


def finish(loss, ug, ig, loss_out, ug_out, ig_out, vl, sem):
    out = [pltpu.make_async_copy(a, b, sem.at[k]) for k, (a, b) in enumerate(((ig, ig_out), (ug, ug_out)))]
    for copy in out:
        copy.start()
    for copy in out:
        copy.wait()
    pltpu.sync_copy(loss, vl)
    loss_out[...] = vl[0, 0:OWN]


def local(users, items, pos_ids):
    V = pltpu.VMEM
    D = pltpu.SemaphoreType.DMA
    I16 = jnp.int16
    HE = E // 2
    HU = NZ // 2 * OWN
    scratch = [
        V((NY * NZ, ROW, E), BF16),
        V((NX * NC, ITM, E), BF16),
        V((1, OWN), jnp.int32),
        V((NY * NZ, 1, 128), jnp.int32),
        V((E, NX * NC * ITM), BF16),
        V((NY, E, CH), BF16),
        V((NY, 2, 1, CH), F32),
        V((2 * ITM, CH), F32),
        V((2 * ITM, CH), F32),
        V((NX * NC, NY, ITM, CH), F32),
        V((NY, NX * NC, 1, CH), F32),
        V((NY, NX * NC, 1, CH), F32),
        V((NY, NX * NC, 1, CH), F32),
        V((NC, NX, ITM, NY * CH), BF16),
        V((16, 128), F32),
        V((NY, 8, 128), F32),
        V((NY, 16, 128), F32),
        V((NY, 8, 128), F32),
        V((NZ, 16, 128), F32),
        V((NZ, 8, 128), F32),
        V((NY, 1, CH), F32),
        V((NY, NZ, ROW, E), F32),
        V((2, HU, E), I16), V((2, 1, E), F32),
        V((4, HU, E), I16), V((4, 1, E), F32),
        V((2, HU, E), I16), V((2, 1, E), F32),
        V((4, HU, E), I16), V((4, 1, E), F32),
        V((NZ, OWN, E), I16), V((NZ, 1, E), F32),
        V((NZ, OWN, E), I16), V((NZ, 1, E), F32),
        V((NX * NC, ITM, E), F32),
        V((NX, ITM, E), I16), V((NX, 1, E), F32),
        V((NX, ITM, E), I16), V((NX, 1, E), F32),
        V((2, HE, E), I16), V((2, 1, E), F32),
        V((4, HE, E), I16), V((4, 1, E), F32),
        V((2, HE, E), I16), V((2, 1, E), F32),
        V((4, HE, E), I16), V((4, 1, E), F32),
        V((1, 128), F32), V((OWN, E), F32), V((ITM, E), F32),
        D((3,)),
        D((4,)),
        D((1,)),
        D((1,)),
        D((1,)),
        D((NY * NZ,)),
        D((2 * NX * NC,)),
        D((1,)), D((1,)), D((1,)), D((1,)),
        D((2, 2)), D((1, 2)), D((1, 2)), D((NX, 2)), D((2, 2)), D((1, 2)),
    ]
    outs = (
        jax.ShapeDtypeStruct((1, 128), F32),
        jax.ShapeDtypeStruct((OWN, E), F32),
        jax.ShapeDtypeStruct((ITM, E), F32),
    )
    hbm = pl.BlockSpec(memory_space=pltpu.HBM)
    loss, ug, ig = pl.pallas_call(
        kernel,
        out_shape=tuple(pltpu.VMEM(o.shape, o.dtype) for o in outs),
        in_specs=[hbm] * 3,
        out_specs=tuple([pl.BlockSpec(memory_space=pltpu.VMEM)] * 3),
        scratch_shapes=scratch,
        compiler_params=pltpu.CompilerParams(
            collective_id=0, has_side_effects=True, vmem_limit_bytes=40 * 2**20
        ),
        name="infonce",
    )(*(pltpu.with_memory_space_constraint(a, pltpu.HBM) for a in (users, items, pos_ids.reshape(1, OWN))))
    return pl.pallas_call(
        finish,
        out_shape=(jax.ShapeDtypeStruct((OWN,), F32), *outs[1:]),
        in_specs=[pl.BlockSpec(memory_space=pl.ANY)] * 3,
        out_specs=(pl.BlockSpec(memory_space=pltpu.VMEM), hbm, hbm),
        scratch_shapes=[V((1, 128), F32), D((2,))],
        compiler_params=pltpu.CompilerParams(vmem_limit_bytes=2**20),
        name="finish",
    )(loss, ug, ig)


def solution(mesh):
    torus = Mesh(mesh.devices.reshape(2, NZ, 2, NY, NC), AXES)
    every = P(AXES)
    return jax.shard_map(
        local,
        mesh=torus,
        in_specs=(P(AXES, None), P(AXES, None), every),
        out_specs=(every, P(AXES, None), P(AXES, None)),
        check_vma=False,
    )
```
